128 devices in a mesh: group: 4 (over x), member: 32 (over y, z, core).
Axes of the slice: x: 4, y: 4, z: 4, core: 2. Of those that a mesh axis runs over, the one named last changes fastest.
Arguments:
- features: bfloat16 [524288, 128], P(('group', 'member')), may hold values from -6 to 6
- history: bfloat16 [524288, 128], P(('group', 'member')), may hold values from -6 to 6
- tiles: bfloat16 [65536, 128, 128], P(('group', 'member'))
- tile_src: int32 [4096, 16], P(('group', 'member')), may hold values from 0 to 71
- degree: int32 [524288], P(('group', 'member')), may hold values from 8 to 128
- boundary_rows: int32 [128, 256], P(('group', 'member')), may hold values from 0 to 4095
- picks: int32 [4096, 1], P(('group', 'member')), may hold values from 0 to 1
- stale_rows: int32 [512, 256], P(('group', 'member')), may hold values from 0 to 4095
- w_self: bfloat16 [128, 128], replicated, may hold values from -0.5 to 0.5
- w_neigh: bfloat16 [128, 128], replicated, may hold values from -0.5 to 0.5
- cotangent: bfloat16 [524288, 128], P(('group', 'member')), may hold values from -6 to 6
Outputs:
- layer_out: bfloat16 [524288, 128], P(('group', 'member'))
- grad_features: bfloat16 [524288, 128], P(('group', 'member'))
- grad_self: float32 [128, 128], replicated
- grad_neigh: float32 [128, 128], replicated
The draws below stay inside these ranges and needn't reach their ends.
Inputs may be any that keep to these rules, and one draw needn't show every extreme that they name: `boundary_rows`: local row indices of the sending device. `stale_rows`: local row indices of the sending device, one list for each destination group. `tile_src`: indices into the device's source blocks: own blocks, then taken boundary blocks member by member, then historical blocks group by group. `degree`: a normalizer given with the graph, not derived from the tiles.
All inputs are finite; a program needn't handle non-finite values.
Results may differ from the reference program's by a relative error of at most 0.0051.
Values may be sent and summed in bfloat16 or wider, within the bound.
No kernel may reach another device: no remote copies, remote signals or barrier semaphores. Data moves between devices by JAX's collectives and lax.ppermute only.
A program may use at most 192 MiB of HBM per device.

```python
import jax
import jax.numpy as jnp
from jax import lax

WIDTH = 128
OUT_WIDTH = 128
TILE = 128
BLOCKS_DEV = 32
TILES_ROW = 16
PICKED = 1
BOUNDARY = 2
STALE = 2
NODES_DEV = 4096
NODES = 524288
BLOCKS = 4096
SOURCES = 72
N_GROUP = 4
N_MEMBER = 32
DEVICES = 128


def draw_tiles(key, part):
    first, second = jax.random.split(jax.random.fold_in(key, 17))
    shape = (BLOCKS * TILES_ROW, TILE, TILE)
    density = 0.0625
    values = jax.random.uniform(second, shape, jnp.float32, 0.5, 1.5)
    keep = jax.random.uniform(first, shape, jnp.float32) < density
    return jnp.where(keep, values, 0.0).astype(jnp.bfloat16)


def plant(drawn, rng, low, largest):
    index_at = [jax.random.randint(jax.random.fold_in(rng, axis), (), 0, length) for axis, length in enumerate(drawn.shape)]
    main_axis = drawn.shape.index(max(drawn.shape))
    next_to = index_at[:main_axis] + [(index_at[main_axis] + 1) % drawn.shape[main_axis]] + index_at[main_axis + 1:]
    return drawn.at[tuple(index_at)].set(low).at[tuple(next_to)].set(largest)


def block_scale(stream_key, dims, shards, low, top_value):
    gain, own = 1.0, jax.random.fold_in(stream_key, 6)
    for position, shards_of in shards:
        heights = jnp.exp(jax.random.uniform(jax.random.fold_in(own, position), (shards_of,), jnp.float32, low / len(shards), top_value / len(shards)))
        gain = gain * jnp.repeat(heights, dims[position] // shards_of).reshape([-1 if axis == position else 1 for axis in range(len(dims))])
    return gain


def noise(rng, dims, width, most, cuts=(), kind=jnp.bfloat16):
    values = jax.random.normal(rng, dims, jnp.float32) * width
    if len(cuts) > 0:
        values = block_scale(rng, dims, cuts, -0.22, 0.18) * values
    return jnp.clip(values, min=-most, max=most).astype(kind)


def setup_inputs(seed: int = 0) -> dict:
    splits = jax.random.split(jax.random.key(seed), 12)
    features = noise(splits[0], (NODES, WIDTH), 1.0, 6.0, ((0, 128),))
    history = noise(splits[1], (NODES, WIDTH), 1.0, 6.0, ((0, 128),))
    tiles = draw_tiles(jax.random.fold_in(splits[11], 71), 0)
    tile_src = plant(jax.random.randint(splits[3], (BLOCKS, TILES_ROW), 0, SOURCES), jax.random.fold_in(splits[3], 1), 0, SOURCES - 1).astype(jnp.int32)
    degree = plant(jax.random.randint(splits[4], (NODES,), 8, 129), jax.random.fold_in(splits[4], 1), 8, 128).astype(jnp.int32)
    boundary_rows = plant(jax.random.randint(splits[5], (DEVICES, BOUNDARY * TILE), 0, NODES_DEV), jax.random.fold_in(splits[5], 1), 0, NODES_DEV - 1).astype(jnp.int32)
    picks = plant(jax.random.randint(splits[6], (DEVICES * N_MEMBER, PICKED), 0, BOUNDARY), jax.random.fold_in(splits[6], 1), 0, BOUNDARY - 1).astype(jnp.int32)
    stale_rows = plant(jax.random.randint(splits[7], (DEVICES * N_GROUP, STALE * TILE), 0, NODES_DEV), jax.random.fold_in(splits[7], 1), 0, NODES_DEV - 1).astype(jnp.int32)
    w_self = noise(splits[8], (WIDTH, OUT_WIDTH), WIDTH ** -0.5, 0.5)
    w_neigh = noise(splits[9], (WIDTH, OUT_WIDTH), WIDTH ** -0.5, 0.5)
    cotangent = noise(splits[10], (NODES, OUT_WIDTH), 1.0, 6.0, ((0, 128),))
    return dict(features=features, history=history, tiles=tiles, tile_src=tile_src, degree=degree, boundary_rows=boundary_rows, picks=picks, stale_rows=stale_rows, w_self=w_self, w_neigh=w_neigh, cotangent=cotangent)


def reference(features, history, tiles, tile_src, degree, boundary_rows, picks, stale_rows, w_self, w_neigh, cotangent):
    groups = N_GROUP
    members = N_MEMBER
    devs = groups * members
    feats = features.reshape(devs, NODES_DEV, WIDTH)
    hists = history.reshape(devs, NODES_DEV, WIDTH)
    brows = boundary_rows.reshape(devs, BOUNDARY * TILE)
    bound = jax.vmap(lambda table, rows: table[rows])(feats, brows).reshape(devs, BOUNDARY, TILE, WIDTH)
    chosen = picks.reshape(devs, members, PICKED)
    group_of = jnp.arange(devs, dtype=jnp.int32) // members
    owner = group_of[:, None] * members + jnp.arange(members, dtype=jnp.int32)[None, :]
    halo = bound[owner[:, :, None], chosen]
    srows = stale_rows.reshape(devs, groups, STALE * TILE)
    sent = jax.vmap(lambda table, rows: table[rows])(hists, srows)
    sent = sent.reshape(groups, members, groups, STALE, TILE, WIDTH)
    stale = sent.transpose(2, 1, 0, 3, 4, 5).reshape(devs, groups * STALE, TILE, WIDTH)
    sources = jnp.concatenate([feats.reshape(devs, BLOCKS_DEV, TILE, WIDTH), halo.reshape(devs, members * PICKED, TILE, WIDTH), stale], axis=1)
    tiled = tiles.reshape(devs, BLOCKS_DEV, TILES_ROW, TILE, TILE)
    src_index = tile_src.reshape(devs, BLOCKS_DEV, TILES_ROW)
    degs = degree.reshape(devs, NODES_DEV, 1).astype(jnp.float32)
    cots = cotangent.reshape(devs, NODES_DEV, OUT_WIDTH)

    def one_device(args):
        srcs, tl, idx, dg, own, cot = args
        picked = srcs[idx]
        summed = jnp.einsum('btij,btjf->bif', tl.astype(jnp.float32), picked.astype(jnp.float32))
        agg = (summed.reshape(NODES_DEV, WIDTH) / dg).astype(jnp.bfloat16)
        pre = jnp.dot(own, w_self, preferred_element_type=jnp.float32) + jnp.dot(agg, w_neigh, preferred_element_type=jnp.float32)
        scale_row = lax.rsqrt(lax.optimization_barrier(jnp.mean(pre * pre, axis=-1, keepdims=True)) + 1e-05)
        out = (pre * scale_row).astype(jnp.bfloat16)
        grad_out = cot.astype(jnp.float32)
        dpre = (scale_row * grad_out - pre * scale_row ** 3 * lax.optimization_barrier(jnp.mean(grad_out * pre, axis=-1, keepdims=True))).astype(jnp.bfloat16)
        part_self = jnp.dot(own.T, dpre, preferred_element_type=jnp.float32)
        part_neigh = jnp.dot(agg.T, dpre, preferred_element_type=jnp.float32)
        dself = jnp.dot(dpre, w_self.T, preferred_element_type=jnp.float32)
        back = (jnp.dot(dpre, w_neigh.T, preferred_element_type=jnp.float32) / dg).astype(jnp.bfloat16)
        back = back.reshape(BLOCKS_DEV, TILE, WIDTH)
        per_tile = jnp.einsum('btij,bif->btjf', tl.astype(jnp.float32), back.astype(jnp.float32))
        src_grad = jnp.zeros((SOURCES, TILE, WIDTH), jnp.float32).at[idx.reshape(-1)].add(per_tile.reshape(-1, TILE, WIDTH))
        return (out, part_self, part_neigh, dself, src_grad[:BLOCKS_DEV + members * PICKED])
    outs, parts_self, parts_neigh, dselfs, src_grads = lax.map(one_device, (sources, tiled, src_index, degs, feats, cots))
    factor = NODES ** (-0.5)
    grad_self = lax.optimization_barrier(jnp.sum(parts_self, axis=0)) * factor
    grad_neigh = lax.optimization_barrier(jnp.sum(parts_neigh, axis=0)) * factor
    local_grad = src_grads[:, :BLOCKS_DEV].reshape(devs, NODES_DEV, WIDTH)
    halo_grad = src_grads[:, BLOCKS_DEV:].reshape(devs, members, PICKED, TILE, WIDTH)
    bound_grad = jnp.zeros((devs, BOUNDARY, TILE, WIDTH), jnp.float32).at[owner[:, :, None], chosen].add(halo_grad)
    row_grad = dselfs + local_grad
    row_grad = jax.vmap(lambda grads, rows, extra: grads.at[rows].add(extra.reshape(-1, WIDTH)))(row_grad, brows, bound_grad)
    layer_out = outs.reshape(NODES, OUT_WIDTH)
    grad_features = row_grad.reshape(NODES, WIDTH).astype(jnp.bfloat16)
    return (layer_out, grad_features, grad_self, grad_neigh)
```

```python
import functools
import math

import jax
import jax.numpy as jnp
from jax import lax
from jax.experimental import pallas as pl
from jax.experimental.pallas import tpu as pltpu
from jax.sharding import PartitionSpec as P

F32 = jnp.float32
BF16 = jnp.bfloat16
MIB = 1024 * 1024


def exchange(value, axis):
    return lax.all_to_all(value, axis, split_axis=0, concat_axis=0, tiled=True)


def any_spec():
    return pl.BlockSpec(memory_space=pl.ANY)


def column(row, lanes):
    return jnp.broadcast_to(row, (lanes, lanes)).T


def gather_kernel(rows_ref, table_ref, out_ref):
    count = rows_ref.shape[0]
    nodes, lanes = table_ref.shape
    wide = 256
    col = jnp.concatenate([column(rows_ref[k], lanes) for k in range(count)], axis=0)
    lane = lax.broadcasted_iota(jnp.int32, (count * lanes, lanes), 1)
    off = col - lane
    acc = jnp.zeros((count * lanes, lanes), F32)
    for c in range(nodes // wide):
        hot = jnp.concatenate(
            [
                jnp.where(off == c * wide + k * lanes, F32(1), F32(0)).astype(BF16)
                for k in range(wide // lanes)
            ],
            axis=1,
        )
        acc += jnp.dot(hot, table_ref[c * wide : (c + 1) * wide, :], preferred_element_type=F32)
    out_ref[...] = acc.astype(BF16)


def gather_rows(rows, table, name):
    width = table.shape[1]
    step = 256
    total = rows.shape[0]
    return pl.pallas_call(
        gather_kernel,
        grid=(total // step,),
        in_specs=[
            pl.BlockSpec((step // 128, 1, 128), lambda i: (i, 0, 0)),
            pl.BlockSpec(table.shape, lambda i: (0, 0)),
        ],
        out_specs=pl.BlockSpec((step, width), lambda i: (i, 0)),
        out_shape=jax.ShapeDtypeStruct((total, width), table.dtype),
        name=name,
    )(rows.reshape(-1, 1, 128), table)


def forward_kernel(
    src_ref, tiles_ref, own_ref, halo_ref, stale_ref, feat_ref, deg_ref, cot_ref, w_ref, wn_ref,
    out_ref, dpre_t_ref, back_t_ref, part_ref,
    sources, part_acc, sems, *, per_step, tiles_row,
):
    step = pl.program_id(0)
    tile = feat_ref.shape[1]
    own, halo, stale = own_ref.shape[0], halo_ref.shape[0], stale_ref.shape[0]

    @pl.when(step == 0)
    def _():
        copies = [
            pltpu.make_async_copy(own_ref, sources.at[pl.ds(0, own)], sems.at[0]),
            pltpu.make_async_copy(halo_ref, sources.at[pl.ds(own, halo)], sems.at[1]),
            pltpu.make_async_copy(stale_ref, sources.at[pl.ds(own + halo, stale)], sems.at[2]),
        ]
        for c in copies:
            c.start()
        part_acc[...] = jnp.zeros_like(part_acc)
        for c in copies:
            c.wait()

    inv_rows, both, dpres = [], [], []
    for k in range(per_step):
        block = step * per_step + k
        lhs = jnp.concatenate([tiles_ref[k * tiles_row + t] for t in range(tiles_row)], axis=1)
        rhs = jnp.concatenate(
            [sources[src_ref[block * tiles_row + t]] for t in range(tiles_row)], axis=0
        )
        summed = jnp.dot(lhs, rhs, preferred_element_type=F32)
        inv = 1.0 / deg_ref[k].astype(F32)
        agg = (summed * column(inv, tile)).astype(BF16)
        x = jnp.concatenate([feat_ref[k], agg], axis=1)
        pre = jnp.dot(x, w_ref[...], preferred_element_type=F32)
        scale = lax.rsqrt(jnp.mean(pre * pre, axis=-1, keepdims=True) + 1e-05)
        out_ref[k] = (pre * scale).astype(BF16)
        grad = cot_ref[k].astype(F32)
        mix = jnp.mean(grad * pre, axis=-1, keepdims=True)
        dpre = scale * grad - pre * (scale * scale * scale * mix)
        inv_rows.append(inv)
        both.append(x)
        dpres.append(dpre.T.astype(BF16))
    dpre_t = jnp.concatenate(dpres, axis=1)
    inv_row = jnp.concatenate(inv_rows, axis=1)
    back = jnp.dot(wn_ref[...], dpre_t, preferred_element_type=F32) * inv_row
    part_acc[...] += jnp.dot(dpre_t, jnp.concatenate(both, axis=0), preferred_element_type=F32)
    for k in range(per_step):
        dpre_t_ref[k] = dpres[k]
        back_t_ref[k] = back[:, k * tile : (k + 1) * tile].astype(BF16)

    @pl.when(step == pl.num_programs(0) - 1)
    def _():
        width = feat_ref.shape[2]
        part_ref[:width, :] = part_acc[:, :width].T
        part_ref[width:, :] = part_acc[:, width:].T


def forward(src, tiles, own, halo, stale, degree, cot, w_cat, w_neigh, per_step=2):
    blocks, tile, width = own.shape
    tiles_row = tiles.shape[0] // blocks
    node = pl.BlockSpec((per_step, tile, width), lambda i, s: (i, 0, 0))
    return pl.pallas_call(
        functools.partial(forward_kernel, per_step=per_step, tiles_row=tiles_row),
        grid_spec=pltpu.PrefetchScalarGridSpec(
            num_scalar_prefetch=1,
            grid=(blocks // per_step,),
            in_specs=[
                pl.BlockSpec((per_step * tiles_row, tile, tile), lambda i, s: (i, 0, 0)),
                any_spec(),
                any_spec(),
                any_spec(),
                node,
                pl.BlockSpec((per_step, 1, tile), lambda i, s: (i, 0, 0)),
                node,
                pl.BlockSpec(w_cat.shape, lambda i, s: (0, 0)),
                pl.BlockSpec(w_neigh.shape, lambda i, s: (0, 0)),
            ],
            out_specs=[node, node, node, pl.BlockSpec((2 * width, width), lambda i, s: (0, 0))],
            scratch_shapes=[
                pltpu.VMEM((own.shape[0] + halo.shape[0] + stale.shape[0], tile, width), BF16),
                pltpu.VMEM((width, 2 * width), F32),
                pltpu.SemaphoreType.DMA((3,)),
            ],
        ),
        out_shape=[
            jax.ShapeDtypeStruct(own.shape, BF16),
            jax.ShapeDtypeStruct(own.shape, BF16),
            jax.ShapeDtypeStruct(own.shape, BF16),
            jax.ShapeDtypeStruct((2 * width, width), F32),
        ],
        compiler_params=pltpu.CompilerParams(dimension_semantics=("arbitrary",)),
        name="forward",
    )(src, tiles, own, halo, stale, own, degree, cot, w_cat, w_neigh)


def backward_kernel(
    src_ref, tiles_ref, back_ref, halo_ref, own_ref, acc, *, per_step, tiles_row
):
    step = pl.program_id(0)
    own = own_ref.shape[0]
    halo = halo_ref.shape[0]
    tile = back_ref.shape[2]

    @pl.when(step == 0)
    def _():
        acc[...] = jnp.zeros_like(acc)

    for k in range(per_step):
        back = back_ref[k]
        block = step * per_step + k
        for t in range(0, tiles_row, 2):
            at = k * tiles_row + t
            pair = jnp.concatenate([tiles_ref[at], tiles_ref[at + 1]], axis=1)
            got = jnp.dot(back, pair, preferred_element_type=F32)
            for u in range(2):
                s = src_ref[block * tiles_row + t + u]
                acc[s] += got[:, u * tile : (u + 1) * tile]

    @pl.when(step == pl.num_programs(0) - 1)
    def _():
        own_ref[...] = acc[:own]
        halo_ref[...] = acc[own : own + halo].astype(BF16)


def backward(src, tiles, back_t, halo, count, per_step=2):
    blocks, width, tile = back_t.shape
    tiles_row = tiles.shape[0] // blocks
    return pl.pallas_call(
        functools.partial(backward_kernel, per_step=per_step, tiles_row=tiles_row),
        grid_spec=pltpu.PrefetchScalarGridSpec(
            num_scalar_prefetch=1,
            grid=(blocks // per_step,),
            in_specs=[
                pl.BlockSpec((per_step * tiles_row, tile, tile), lambda i, s: (i, 0, 0)),
                pl.BlockSpec((per_step, width, tile), lambda i, s: (i, 0, 0)),
            ],
            out_specs=[
                pl.BlockSpec((halo, width, tile), lambda i, s: (0, 0, 0)),
                pl.BlockSpec((blocks, width, tile), lambda i, s: (0, 0, 0)),
            ],
            scratch_shapes=[pltpu.VMEM((count, width, tile), F32)],
        ),
        out_shape=[
            jax.ShapeDtypeStruct((halo, width, tile), BF16),
            jax.ShapeDtypeStruct((blocks, width, tile), F32),
        ],
        compiler_params=pltpu.CompilerParams(dimension_semantics=("arbitrary",)),
        name="backward",
    )(src, tiles, back_t)


def local_kernel(acc_ref, dpre_ref, w_ref, out_ref):
    per, width, tile = acc_ref.shape
    for k in range(per):
        both = acc_ref[k] + jnp.dot(w_ref[...], dpre_ref[k], preferred_element_type=F32)
        out_ref[k * tile : (k + 1) * tile, :] = both.T


def local_rows(acc, dpre_t, w_self, per_step=8):
    blocks, width, tile = acc.shape
    block = pl.BlockSpec((per_step, width, tile), lambda i: (i, 0, 0))
    return pl.pallas_call(
        local_kernel,
        grid=(blocks // per_step,),
        in_specs=[block, block, pl.BlockSpec(w_self.shape, lambda i: (0, 0))],
        out_specs=pl.BlockSpec((per_step * tile, width), lambda i: (i, 0)),
        out_shape=jax.ShapeDtypeStruct((blocks * tile, width), F32),
        name="local_rows",
    )(acc, dpre_t, w_self)


def final_kernel(wanted_ref, returned_ref, rows_ref, local_ref, out_ref, spread, *, offered):
    step = pl.program_id(0)
    per, width = local_ref.shape
    members, _, tile = returned_ref.shape

    @pl.when(step == 0)
    def _():
        sums = []
        for k in range(offered):
            total = jnp.zeros((width, tile), F32)
            for p in range(members):
                block = returned_ref[p].astype(F32)
                total += jnp.where(wanted_ref[p] == k, block, F32(0))
            sums.append(total.T)
        grad = jnp.concatenate(sums, axis=0)
        high = grad.astype(BF16)
        spread[:, :width] = high
        spread[:, width:] = (grad - high.astype(F32)).astype(BF16)

    at = lax.broadcasted_iota(jnp.int32, (per, offered * tile), 0) + step * per
    hot = jnp.where(at == rows_ref[...], F32(1), F32(0)).astype(BF16)
    more = jnp.dot(hot, spread[...], preferred_element_type=F32)
    out_ref[...] = (local_ref[...] + (more[:, :width] + more[:, width:])).astype(BF16)


def final(wanted, returned, rows, local, offered, per_step=1024):
    nodes, width = local.shape
    tile = returned.shape[2]
    return pl.pallas_call(
        functools.partial(final_kernel, offered=offered),
        grid_spec=pltpu.PrefetchScalarGridSpec(
            num_scalar_prefetch=1,
            grid=(nodes // per_step,),
            in_specs=[
                pl.BlockSpec(returned.shape, lambda i, s: (0, 0, 0)),
                pl.BlockSpec(rows.shape, lambda i, s: (0, 0)),
                pl.BlockSpec((per_step, width), lambda i, s: (i, 0)),
            ],
            out_specs=pl.BlockSpec((per_step, width), lambda i, s: (i, 0)),
            scratch_shapes=[pltpu.VMEM((offered * tile, 2 * width), BF16)],
        ),
        out_shape=jax.ShapeDtypeStruct((nodes, width), BF16),
        compiler_params=pltpu.CompilerParams(dimension_semantics=("arbitrary",)),
        name="final",
    )(wanted, returned, rows, local)


def on_device(
    features,
    history,
    tiles,
    tile_src,
    degree,
    boundary_rows,
    picks,
    stale_rows,
    w_self,
    w_neigh,
    cotangent,
):
    members = lax.axis_size("member")
    groups = lax.axis_size("group")
    tile = tiles.shape[1]
    width = features.shape[1]
    blocks = features.shape[0] // tile
    offered = boundary_rows.shape[1] // tile
    taken = picks.shape[1]
    src = tile_src.reshape(-1)
    wanted = exchange(picks, "member").reshape(-1)
    bound = gather_rows(boundary_rows[0], features, "gather_bound").reshape(offered, tile, width)
    sent = gather_rows(stale_rows.reshape(-1), history, "gather_stale")
    outgoing = bound[0][None]
    for k in range(1, offered):
        outgoing = jnp.where((wanted == k)[:, None, None], bound[k][None], outgoing)
    halo = exchange(outgoing, "member")
    stale = exchange(sent.reshape(groups, -1, width), "group").reshape(-1, tile, width)
    own = features.reshape(blocks, tile, width)
    out, dpre_t, back_t, part = forward(
        src,
        tiles,
        own,
        halo,
        stale,
        degree.reshape(blocks, 1, tile),
        cotangent.reshape(blocks, tile, width),
        jnp.concatenate([w_self, w_neigh], axis=0),
        w_neigh,
    )
    share = exchange(part.reshape(members, -1, width), "member").sum(axis=0)
    count = blocks + members * taken + stale.shape[0]
    halo_grad, own_grad = backward(src, tiles, back_t, members * taken, count)
    returned = exchange(halo_grad, "member")
    everyone = jnp.broadcast_to(share, (groups * members, *share.shape))
    shares = exchange(everyone, ("group", "member"))
    full = shares.reshape(groups, -1, width).sum(axis=0)
    local = local_rows(own_grad, dpre_t, w_self)
    grad_features = final(wanted, returned, boundary_rows, local, offered)
    factor = 1.0 / math.sqrt(features.shape[0] * members * groups)
    full = full * factor
    return (out.reshape(-1, width), grad_features, full[:width], full[width:])


def solution(mesh):
    placed = (
        P(("group", "member"), None),
        P(("group", "member"), None),
        P(("group", "member"), None, None),
        P(("group", "member"), None),
        P(("group", "member")),
        P(("group", "member"), None),
        P(("group", "member"), None),
        P(("group", "member"), None),
        P(),
        P(),
        P(("group", "member"), None),
    )
    return jax.shard_map(
        on_device,
        mesh=mesh,
        in_specs=placed,
        out_specs=(P(("group", "member"), None), P(("group", "member"), None), P(), P()),
        check_vma=False,
    )
```

```python
import functools
import math

import jax
import jax.numpy as jnp
from jax import lax
from jax.experimental import pallas as pl
from jax.experimental.pallas import tpu as pltpu
from jax.sharding import PartitionSpec as P

F32 = jnp.float32
BF16 = jnp.bfloat16
MIB = 1024 * 1024


def exchange(value, axis):
    return lax.all_to_all(value, axis, split_axis=0, concat_axis=0, tiled=True)


def any_spec():
    return pl.BlockSpec(memory_space=pl.ANY)


def column(row, lanes):
    return jnp.broadcast_to(row, (lanes, lanes)).T


def picked_rows(rows, table_ref):
    nodes, lanes = table_ref.shape
    wide = 256
    col = jnp.concatenate([column(r, lanes) for r in rows], axis=0)
    off = col - lax.broadcasted_iota(jnp.int32, col.shape, 1)
    acc = jnp.zeros(col.shape, F32)
    for c in range(nodes // wide):
        hot = jnp.concatenate(
            [
                jnp.where(off == c * wide + k * lanes, F32(1), F32(0)).astype(BF16)
                for k in range(wide // lanes)
            ],
            axis=1,
        )
        acc += jnp.dot(hot, table_ref[c * wide : (c + 1) * wide, :], preferred_element_type=F32)
    return acc.astype(BF16)


def bound_kernel(rows_ref, table_ref, out_ref, halves, sems, *, tile):
    offered = rows_ref.shape[1] // tile
    got = picked_rows([rows_ref[:, k * tile : (k + 1) * tile] for k in range(offered)], table_ref)
    half = tile // 2
    for c in range(2):
        for k in range(offered):
            halves[c, k] = got[k * tile + c * half : k * tile + (c + 1) * half]
    copies = [
        pltpu.make_async_copy(halves.at[p % 2], out_ref.at[p], sems.at[p])
        for p in range(out_ref.shape[0])
    ]
    for c in copies:
        c.start()
    for c in copies:
        c.wait()


def bound_halves(rows, table, members, tile):
    offered = rows.shape[1] // tile
    width = table.shape[1]
    return pl.pallas_call(
        functools.partial(bound_kernel, tile=tile),
        out_specs=any_spec(),
        out_shape=jax.ShapeDtypeStruct((members, offered, tile // 2, width), BF16),
        scratch_shapes=[
            pltpu.VMEM((2, offered, tile // 2, width), BF16),
            pltpu.SemaphoreType.DMA((members,)),
        ],
        name="bound_halves",
    )(rows, table)


def stale_kernel(rows_ref, table_ref, out_ref):
    lanes = table_ref.shape[1]
    count = rows_ref.shape[1] // lanes
    for g in range(rows_ref.shape[0]):
        rows = [rows_ref[g : g + 1, k * lanes : (k + 1) * lanes] for k in range(count)]
        out_ref[g] = picked_rows(rows, table_ref)


def stale_rows_sent(rows, table):
    return pl.pallas_call(
        stale_kernel,
        out_shape=jax.ShapeDtypeStruct((*rows.shape, table.shape[1]), BF16),
        name="stale_rows_sent",
    )(rows, table)


def forward_kernel(
    src_ref, picks_ref, core_ref, tiles_ref, own_ref, near_ref, far_ref, stale_ref, deg_ref,
    cot_ref, ws_ref, wn_ref,
    out_ref, dpre_t_ref, back_t_ref, part_ref,
    tiles, sources, cots, aggs, outs, dpre_ts, back_ts, w_cat, inv, part_acc,
    tile_sems, in_sems, out_sems, *, group,
):
    blocks, tile, width = own_ref.shape
    tiles_row = src_ref.shape[0]
    members, offered, half, _ = near_ref.shape
    halo = members * offered
    stale = stale_ref.shape[0]
    core = core_ref[0]

    def tile_copy(b):
        at = pl.ds(b * tiles_row, tiles_row)
        return pltpu.make_async_copy(tiles_ref.at[at], tiles.at[at], tile_sems.at[b])

    def halo_rows(which):
        return sources.at[pl.ds(blocks, halo), pl.ds(pl.multiple_of(which * half, half), half)]

    ins = [
        pltpu.make_async_copy(own_ref, sources.at[pl.ds(0, blocks)], in_sems.at[0]),
        pltpu.make_async_copy(near_ref.reshape(halo, half, width), halo_rows(core), in_sems.at[1]),
        pltpu.make_async_copy(far_ref.reshape(halo, half, width), halo_rows(1 - core), in_sems.at[2]),
        pltpu.make_async_copy(stale_ref, sources.at[pl.ds(blocks + halo, stale)], in_sems.at[3]),
        pltpu.make_async_copy(cot_ref, cots, in_sems.at[4]),
    ]
    for c in ins[:4]:
        c.start()

    @pl.loop(0, blocks)
    def _(b):
        tile_copy(b).start()

    ins[4].start()
    w_cat[:width, :] = ws_ref[...]
    w_cat[width:, :] = wn_ref[...]
    inv[...] = 1.0 / deg_ref[...].astype(F32)
    part_acc[...] = jnp.zeros_like(part_acc)
    for c in ins[:4]:
        c.wait()

    def source_of(b, t):
        s = src_ref[t, b]
        m = jnp.clip(s - blocks, 0, members - 1)
        near = blocks + m * offered + picks_ref[0, m]
        return jnp.where(s < blocks, s, jnp.where(s < blocks + members, near, s - members + halo))

    outputs = ((outs, out_ref), (dpre_ts, dpre_t_ref), (back_ts, back_t_ref))

    def out_copies(g):
        at = pl.ds(g * group, group)
        return [
            pltpu.make_async_copy(buf.at[at], ref.at[at], out_sems.at[k, g])
            for k, (buf, ref) in enumerate(outputs)
        ]

    def arrived(g):
        for k in range(group):
            tile_copy(g * group + k).wait()

    def aggregate(g):
        for k in range(group):
            b = g * group + k
            lhs = jnp.concatenate(
                [tiles[b * tiles_row + t] for t in range(tiles_row)], axis=1
            )
            rhs = jnp.concatenate([sources[source_of(b, t)] for t in range(tiles_row)], axis=0)
            summed = jnp.dot(lhs, rhs, preferred_element_type=F32)
            aggs[b] = (summed * column(inv[pl.ds(b, 1), :], tile)).astype(BF16)

    def dense(g):
        at = pl.ds(g * group, group)
        rows = group * tile
        x = jnp.concatenate(
            [sources[at].reshape(rows, width), aggs[at].reshape(rows, width)], axis=1
        )
        pre = jnp.dot(x, w_cat[...], preferred_element_type=F32)
        scale = lax.rsqrt(jnp.mean(pre * pre, axis=-1, keepdims=True) + 1e-05)
        outs[at] = (pre * scale).astype(BF16).reshape(group, tile, width)
        grad = cots[at].reshape(rows, width).astype(F32)
        mix = jnp.mean(grad * pre, axis=-1, keepdims=True)
        dpre = (scale * grad - pre * (scale * scale * scale * mix)).astype(BF16)
        dpre_t = jnp.concatenate(
            [dpre[k * tile : (k + 1) * tile].T for k in range(group)], axis=1
        )
        inv_row = jnp.concatenate([inv[pl.ds(g * group + k, 1), :] for k in range(group)], axis=1)
        back = jnp.dot(wn_ref[...], dpre_t, preferred_element_type=F32) * inv_row
        part_acc[...] += jnp.dot(dpre_t, x, preferred_element_type=F32)
        for k in range(group):
            dpre_ts[g * group + k] = dpre_t[:, k * tile : (k + 1) * tile]
            back_ts[g * group + k] = back[:, k * tile : (k + 1) * tile].astype(BF16)

    last = blocks // group - 1
    arrived(0)
    aggregate(0)
    ins[4].wait()

    @pl.loop(1, last + 1)
    def _(g):
        arrived(g)
        dense(g - 1)
        aggregate(g)
        for c in out_copies(g - 1):
            c.start()

    dense(last)
    for c in out_copies(last):
        c.start()

    each = 2 * width // members
    for q in range(2):
        grad = part_acc[:, q * width : (q + 1) * width].T
        for p in range(members // 2):
            part_ref[q * (members // 2) + p, :each] = grad[p * each : (p + 1) * each]
    for p in range(members):
        part_ref[p, each:] = jnp.full((each, width), picks_ref[0, p].astype(F32), F32)

    @pl.loop(0, blocks // group)
    def _(g):
        for c in out_copies(g):
            c.wait()


def forward(src, picks, core, tiles, own, near, far, stale, degree, cot, w_self, w_neigh, group=4):
    blocks, tile, width = own.shape
    members, offered = near.shape[:2]
    count = blocks + members * offered + stale.shape[0]
    smem = pl.BlockSpec(memory_space=pltpu.SMEM)
    vmem = pl.BlockSpec(memory_space=pltpu.VMEM)
    node = pltpu.VMEM((blocks, tile, width), BF16)
    return pl.pallas_call(
        functools.partial(forward_kernel, group=group),
        in_specs=[smem] * 3 + [any_spec()] * 5 + [vmem, any_spec(), vmem, vmem],
        out_specs=[any_spec()] * 3 + [vmem],
        scratch_shapes=[
            pltpu.VMEM(tiles.shape, BF16),
            pltpu.VMEM((count, tile, width), BF16),
            node,
            node,
            node,
            node,
            node,
            pltpu.VMEM((2 * width, width), BF16),
            pltpu.VMEM((blocks, tile), F32),
            pltpu.VMEM((width, 2 * width), F32),
            pltpu.SemaphoreType.DMA((blocks,)),
            pltpu.SemaphoreType.DMA((5,)),
            pltpu.SemaphoreType.DMA((3, blocks // group)),
        ],
        out_shape=[
            jax.ShapeDtypeStruct(own.shape, BF16),
            jax.ShapeDtypeStruct(own.shape, BF16),
            jax.ShapeDtypeStruct(own.shape, BF16),
            jax.ShapeDtypeStruct((members, 4 * width // members, width), F32),
        ],
        name="forward",
    )(src, picks, core, tiles, own, near, far, stale, degree, cot, w_self, w_neigh)


def backward_kernel(
    src_ref, tiles_ref, back_ref, halo_ref, even_ref, odd_ref, tiles, backs, even, odd, halos,
    tile_sems, in_sem, out_sems, *, group,
):
    blocks, width, tile = back_ref.shape
    tiles_row = src_ref.shape[0]
    halo = halo_ref.shape[0]

    def tile_copy(b):
        at = pl.ds(b * tiles_row, tiles_row)
        return pltpu.make_async_copy(tiles_ref.at[at], tiles.at[at], tile_sems.at[b])

    back_in = pltpu.make_async_copy(back_ref, backs, in_sem)
    back_in.start()

    @pl.loop(0, blocks)
    def _(b):
        tile_copy(b).start()

    @pl.loop(0, even.shape[0])
    def _(s):
        even[s] = jnp.zeros((width, tile), F32)
        odd[s] = jnp.zeros((width, tile), F32)

    back_in.wait()

    @pl.loop(0, blocks, step=group)
    def _(first):
        for k in range(group):
            tile_copy(first + k).wait()
        for k in range(group):
            b = first + k
            back = backs[b]
            for t in range(0, tiles_row, 2):
                at = b * tiles_row + t
                pair = jnp.concatenate([tiles[at], tiles[at + 1]], axis=1)
                got = jnp.dot(back, pair, preferred_element_type=F32)
                even[src_ref[t, b]] += got[:, :tile]
                odd[src_ref[t + 1, b]] += got[:, tile:]

    outs = [
        pltpu.make_async_copy(even.at[pl.ds(0, blocks)], even_ref, out_sems.at[0]),
        pltpu.make_async_copy(odd.at[pl.ds(0, blocks)], odd_ref, out_sems.at[1]),
        pltpu.make_async_copy(halos, halo_ref, out_sems.at[2]),
    ]

    @pl.loop(0, halo, step=4)
    def _(s):
        for k in range(4):
            halos[s + k] = (even[blocks + s + k] + odd[blocks + s + k]).astype(BF16)

    for c in reversed(outs):
        c.start()
    for c in outs:
        c.wait()


def backward(src, tiles, back_t, halo, count, group=4):
    blocks, width, tile = back_t.shape
    grads = jax.ShapeDtypeStruct((blocks, width, tile), F32)
    return pl.pallas_call(
        functools.partial(backward_kernel, group=group),
        in_specs=[pl.BlockSpec(memory_space=pltpu.SMEM), any_spec(), any_spec()],
        out_specs=[any_spec()] * 3,
        scratch_shapes=[
            pltpu.VMEM(tiles.shape, BF16),
            pltpu.VMEM(back_t.shape, BF16),
            pltpu.VMEM((count, width, tile), F32),
            pltpu.VMEM((count, width, tile), F32),
            pltpu.VMEM((halo, width, tile), BF16),
            pltpu.SemaphoreType.DMA((blocks,)),
            pltpu.SemaphoreType.DMA,
            pltpu.SemaphoreType.DMA((3,)),
        ],
        out_shape=[jax.ShapeDtypeStruct((halo, width, tile), BF16), grads, grads],
        name="backward",
    )(src, tiles, back_t)


def local_kernel(even_ref, odd_ref, dpre_ref, w_ref, out_ref):
    blocks, width, tile = even_ref.shape

    @pl.loop(0, blocks, step=4)
    def _(first):
        for k in range(4):
            b = first + k
            both = even_ref[b] + odd_ref[b]
            both += jnp.dot(w_ref[...], dpre_ref[b], preferred_element_type=F32)
            out_ref[pl.ds(b * tile, tile), :] = both.T


def local_rows(even, odd, dpre_t, w_self):
    blocks, width, tile = even.shape
    return pl.pallas_call(
        local_kernel,
        out_shape=jax.ShapeDtypeStruct((blocks * tile, width), F32),
        name="local_rows",
    )(even, odd, dpre_t, w_self)


def final_kernel(
    parts_ref, returned_ref, rows_ref, local_ref, out_ref, spread, outs, sems, *, offered, chunk
):
    nodes, width = local_ref.shape
    members, _, tile = returned_ref.shape
    each = parts_ref.shape[1] // 2
    sums = [jnp.zeros((width, tile), F32) for _ in range(offered)]
    for p in range(members):
        block = returned_ref[p].astype(F32)
        wanted = parts_ref[p, each : each + 1, :]
        for k in range(offered):
            sums[k] += jnp.where(wanted == F32(k), block, F32(0))
    grad = jnp.concatenate([s.T for s in sums], axis=0)
    high = grad.astype(BF16)
    spread[:, :width] = high
    spread[:, width:] = (grad - high.astype(F32)).astype(BF16)
    copies = []
    for c in range(nodes // chunk):
        at = lax.broadcasted_iota(jnp.int32, (chunk, offered * tile), 0) + c * chunk
        hot = jnp.where(at == rows_ref[...], F32(1), F32(0)).astype(BF16)
        more = jnp.dot(hot, spread[...], preferred_element_type=F32)
        rows = slice(c * chunk, (c + 1) * chunk)
        outs[rows, :] = (local_ref[rows, :] + (more[:, :width] + more[:, width:])).astype(BF16)
        at = pl.ds(c * chunk, chunk)
        copies.append(pltpu.make_async_copy(outs.at[at], out_ref.at[at], sems.at[c]))
        copies[-1].start()
    for c in copies:
        c.wait()


def final(parts, returned, rows, local, offered, chunk=512):
    nodes, width = local.shape
    tile = returned.shape[2]
    return pl.pallas_call(
        functools.partial(final_kernel, offered=offered, chunk=chunk),
        out_specs=any_spec(),
        out_shape=jax.ShapeDtypeStruct((nodes, width), BF16),
        scratch_shapes=[
            pltpu.VMEM((offered * tile, 2 * width), BF16),
            pltpu.VMEM((nodes, width), BF16),
            pltpu.SemaphoreType.DMA((nodes // chunk,)),
        ],
        name="final",
    )(parts, returned, rows, local)


def on_device(
    features,
    history,
    tiles,
    tile_src,
    degree,
    boundary_rows,
    picks,
    stale_rows,
    w_self,
    w_neigh,
    cotangent,
):
    members = lax.axis_size("member")
    groups = lax.axis_size("group")
    tile = tiles.shape[1]
    width = features.shape[1]
    blocks = features.shape[0] // tile
    offered = boundary_rows.shape[1] // tile
    src = tile_src.T
    halves = bound_halves(boundary_rows, features, members, tile)
    near = exchange(halves, "member")
    stale_rows, halves = lax.optimization_barrier((stale_rows, halves))
    sent = stale_rows_sent(stale_rows, history)
    near, sent = lax.optimization_barrier((near, sent))
    far = lax.ppermute(near, "member", [(m, m ^ 1) for m in range(members)])
    stale = exchange(sent, "group").reshape(-1, tile, width)
    own = features.reshape(blocks, tile, width)
    core = (lax.axis_index("member") % 2).astype(jnp.int32).reshape(1)
    out, dpre_t, back_t, part = forward(
        src,
        picks.reshape(1, -1),
        core,
        tiles,
        own,
        near,
        far,
        stale,
        degree.reshape(blocks, tile),
        cotangent.reshape(blocks, tile, width),
        w_self,
        w_neigh,
    )
    parts = exchange(part, "member")
    count = blocks + members + stale.shape[0]
    halo_grad, even, odd = backward(src, tiles, back_t, members, count)
    parts, halo_grad, even, odd = lax.optimization_barrier((parts, halo_grad, even, odd))
    returned = exchange(halo_grad, "member")
    factor = 1.0 / math.sqrt(features.shape[0] * members * groups)
    share = parts[:, : parts.shape[1] // 2].sum(axis=0) * factor
    hop = 1
    while hop < groups:
        share += lax.ppermute(share, "group", [(g, g ^ hop) for g in range(groups)])
        hop *= 2
    copies = jnp.broadcast_to(share, (members, *share.shape))
    local = local_rows(even, odd, dpre_t, w_self)
    returned, copies, local = lax.optimization_barrier((returned, copies, local))
    full = exchange(copies, "member").reshape(-1, width)
    grad_features = final(parts, returned, boundary_rows, local, offered)
    grad_self, grad_neigh = full[:width], full[width:]
    return (out.reshape(-1, width), grad_features, grad_self, grad_neigh)


def solution(mesh):
    placed = (
        P(("group", "member"), None),
        P(("group", "member"), None),
        P(("group", "member"), None, None),
        P(("group", "member"), None),
        P(("group", "member")),
        P(("group", "member"), None),
        P(("group", "member"), None),
        P(("group", "member"), None),
        P(),
        P(),
        P(("group", "member"), None),
    )
    return jax.shard_map(
        on_device,
        mesh=mesh,
        in_specs=placed,
        out_specs=(P(("group", "member"), None), P(("group", "member"), None), P(), P()),
        check_vma=False,
    )
```

```python
import functools
import math

import jax
import jax.numpy as jnp
from jax import lax
from jax.experimental import pallas as pl
from jax.experimental.pallas import tpu as pltpu
from jax.sharding import PartitionSpec as P

F32 = jnp.float32
BF16 = jnp.bfloat16
MIB = 1024 * 1024


def exchange(value, axis):
    return lax.all_to_all(value, axis, split_axis=0, concat_axis=0, tiled=True)


def any_spec():
    return pl.BlockSpec(memory_space=pl.ANY)


def column(row, lanes):
    return jnp.broadcast_to(row, (lanes, lanes)).T


def picked_rows(rows, table_ref):
    nodes, lanes = table_ref.shape
    wide = 256
    col = jnp.concatenate([column(r, lanes) for r in rows], axis=0)
    off = col - lax.broadcasted_iota(jnp.int32, col.shape, 1)
    acc = jnp.zeros(col.shape, F32)
    for c in range(nodes // wide):
        hot = jnp.concatenate(
            [
                jnp.where(off == c * wide + k * lanes, F32(1), F32(0)).astype(BF16)
                for k in range(wide // lanes)
            ],
            axis=1,
        )
        acc += jnp.dot(hot, table_ref[c * wide : (c + 1) * wide, :], preferred_element_type=F32)
    return acc.astype(BF16)


def bound_kernel(rows_ref, table_ref, out_ref, halves, sems, *, tile):
    offered = rows_ref.shape[1] // tile
    got = picked_rows([rows_ref[:, k * tile : (k + 1) * tile] for k in range(offered)], table_ref)
    half = tile // 2
    for c in range(2):
        for k in range(offered):
            halves[c, k] = got[k * tile + c * half : k * tile + (c + 1) * half]
    copies = [
        pltpu.make_async_copy(halves.at[p % 2], out_ref.at[p], sems.at[p])
        for p in range(out_ref.shape[0])
    ]
    for c in copies:
        c.start()
    for c in copies:
        c.wait()


def bound_halves(rows, table, members, tile):
    offered = rows.shape[1] // tile
    width = table.shape[1]
    return pl.pallas_call(
        functools.partial(bound_kernel, tile=tile),
        out_specs=any_spec(),
        out_shape=jax.ShapeDtypeStruct((members, offered, tile // 2, width), BF16),
        scratch_shapes=[
            pltpu.VMEM((2, offered, tile // 2, width), BF16),
            pltpu.SemaphoreType.DMA((members,)),
        ],
        name="bound_halves",
    )(rows, table)


def stale_kernel(place_ref, rows_ref, table_ref, *out_refs):
    lanes = table_ref.shape[1]
    count = rows_ref.shape[1] // lanes
    groups = len(out_refs)
    for k in range(groups):
        g = lax.rem(place_ref[1] + k, groups)
        rows = rows_ref[pl.ds(g, 1), :]
        out_refs[k][...] = picked_rows(
            [rows[:, c * lanes : (c + 1) * lanes] for c in range(count)], table_ref
        )


def stale_rows_sent(place, rows, table):
    groups, count = rows.shape
    vmem = pl.BlockSpec(memory_space=pltpu.VMEM)
    piece = jax.ShapeDtypeStruct((count, table.shape[1]), BF16)
    return pl.pallas_call(
        stale_kernel,
        in_specs=[pl.BlockSpec(memory_space=pltpu.SMEM), vmem, vmem],
        out_specs=[vmem] * groups,
        out_shape=[piece] * groups,
        name="stale_rows_sent",
    )(place, rows, table)


def forward_kernel(
    src_ref, picks_ref, place_ref, tiles_ref, own_ref, near_ref, far_ref, deg_ref, cot_ref, ws_ref,
    wn_ref, *refs, group, groups,
):
    stale_refs, refs = refs[:groups], refs[groups:]
    out_ref, dpre_t_ref, back_t_ref, part_ref, *refs = refs
    tiles, sources, cots, aggs, outs, dpre_ts, back_ts, w_cat, inv, part_acc, *refs = refs
    tile_sems, in_sems, out_sems = refs
    blocks, tile, width = own_ref.shape
    tiles_row = src_ref.shape[0]
    members, offered, half, _ = near_ref.shape
    halo = members * offered
    stale = stale_refs[0].shape[0]
    core = place_ref[0]
    here = place_ref[1]

    def tile_copy(b):
        at = pl.ds(b * tiles_row, tiles_row)
        return pltpu.make_async_copy(tiles_ref.at[at], tiles.at[at], tile_sems.at[b])

    def halo_rows(which):
        return sources.at[pl.ds(blocks, halo), pl.ds(pl.multiple_of(which * half, half), half)]

    ins = [
        pltpu.make_async_copy(own_ref, sources.at[pl.ds(0, blocks)], in_sems.at[0]),
        pltpu.make_async_copy(near_ref.reshape(halo, half, width), halo_rows(core), in_sems.at[1]),
        pltpu.make_async_copy(far_ref.reshape(halo, half, width), halo_rows(1 - core), in_sems.at[2]),
        *[
            pltpu.make_async_copy(
                ref, sources.at[pl.ds(blocks + halo + k * stale, stale)], in_sems.at[3 + k]
            )
            for k, ref in enumerate(stale_refs)
        ],
    ]
    cot_in = pltpu.make_async_copy(cot_ref, cots, in_sems.at[3 + groups])
    for c in ins:
        c.start()
    tile_copy(0).start()
    cot_in.start()

    @pl.loop(1, blocks)
    def _(b):
        tile_copy(b).start()

    w_cat[:width, :] = ws_ref[...]
    w_cat[width:, :] = wn_ref[...]
    inv[...] = 1.0 / deg_ref[...].astype(F32)
    part_acc[...] = jnp.zeros_like(part_acc)
    for c in ins:
        c.wait()

    def source_of(b, t):
        s = src_ref[t, b]
        m = jnp.clip(s - blocks, 0, members - 1)
        near = blocks + m * offered + picks_ref[0, m]
        late = jnp.maximum(s - blocks - members, 0)
        from_group = late // stale
        back = here - from_group
        back = jnp.where(back < 0, back + groups, back)
        old = blocks + halo + back * stale + late - from_group * stale
        return jnp.where(s < blocks, s, jnp.where(s < blocks + members, near, old))

    outputs = ((outs, out_ref), (dpre_ts, dpre_t_ref), (back_ts, back_t_ref))

    def out_copies(g):
        at = pl.ds(g * group, group)
        return [
            pltpu.make_async_copy(buf.at[at], ref.at[at], out_sems.at[k, g])
            for k, (buf, ref) in enumerate(outputs)
        ]

    def arrived(g):
        for k in range(group):
            tile_copy(g * group + k).wait()

    def aggregate(g):
        for k in range(group):
            b = g * group + k
            lhs = jnp.concatenate(
                [tiles[b * tiles_row + t] for t in range(tiles_row)], axis=1
            )
            rhs = jnp.concatenate([sources[source_of(b, t)] for t in range(tiles_row)], axis=0)
            summed = jnp.dot(lhs, rhs, preferred_element_type=F32)
            aggs[b] = (summed * column(inv[pl.ds(b, 1), :], tile)).astype(BF16)

    def dense(g):
        at = pl.ds(g * group, group)
        rows = group * tile
        x = jnp.concatenate(
            [sources[at].reshape(rows, width), aggs[at].reshape(rows, width)], axis=1
        )
        pre = jnp.dot(x, w_cat[...], preferred_element_type=F32)
        scale = lax.rsqrt(jnp.mean(pre * pre, axis=-1, keepdims=True) + 1e-05)
        outs[at] = (pre * scale).astype(BF16).reshape(group, tile, width)
        grad = cots[at].reshape(rows, width).astype(F32)
        mix = jnp.mean(grad * pre, axis=-1, keepdims=True)
        dpre = (scale * grad - pre * (scale * scale * scale * mix)).astype(BF16)
        dpre_t = jnp.concatenate(
            [dpre[k * tile : (k + 1) * tile].T for k in range(group)], axis=1
        )
        inv_row = jnp.concatenate([inv[pl.ds(g * group + k, 1), :] for k in range(group)], axis=1)
        back = jnp.dot(wn_ref[...], dpre_t, preferred_element_type=F32) * inv_row
        part_acc[...] += jnp.dot(dpre_t, x, preferred_element_type=F32)
        for k in range(group):
            dpre_ts[g * group + k] = dpre_t[:, k * tile : (k + 1) * tile]
            back_ts[g * group + k] = back[:, k * tile : (k + 1) * tile].astype(BF16)

    last = blocks // group - 1
    arrived(0)
    aggregate(0)
    cot_in.wait()

    @pl.loop(1, last + 1)
    def _(g):
        arrived(g)
        dense(g - 1)
        aggregate(g)
        for c in out_copies(g - 1):
            c.start()

    dense(last)
    for c in out_copies(last):
        c.start()

    each = 2 * width // members
    for q in range(2):
        grad = part_acc[:, q * width : (q + 1) * width].T
        for p in range(members // 2):
            part_ref[q * (members // 2) + p, :each] = grad[p * each : (p + 1) * each]
    for p in range(members):
        part_ref[p, each:] = jnp.full((each, width), picks_ref[0, p].astype(F32), F32)

    @pl.loop(0, blocks // group)
    def _(g):
        for c in out_copies(g):
            c.wait()


def forward(src, picks, place, tiles, own, near, far, stale, degree, cot, w_self, w_neigh, group=4):
    blocks, tile, width = own.shape
    members, offered = near.shape[:2]
    groups = len(stale)
    count = blocks + members * offered + groups * stale[0].shape[0]
    smem = pl.BlockSpec(memory_space=pltpu.SMEM)
    vmem = pl.BlockSpec(memory_space=pltpu.VMEM)
    node = pltpu.VMEM((blocks, tile, width), BF16)
    return pl.pallas_call(
        functools.partial(forward_kernel, group=group, groups=groups),
        in_specs=[smem] * 3 + [any_spec()] * 4 + [vmem, any_spec(), vmem, vmem] + [any_spec()] * groups,
        out_specs=[any_spec()] * 3 + [vmem],
        scratch_shapes=[
            pltpu.VMEM(tiles.shape, BF16),
            pltpu.VMEM((count, tile, width), BF16),
            node,
            node,
            node,
            node,
            node,
            pltpu.VMEM((2 * width, width), BF16),
            pltpu.VMEM((blocks, tile), F32),
            pltpu.VMEM((width, 2 * width), F32),
            pltpu.SemaphoreType.DMA((blocks,)),
            pltpu.SemaphoreType.DMA((4 + groups,)),
            pltpu.SemaphoreType.DMA((3, blocks // group)),
        ],
        out_shape=[
            jax.ShapeDtypeStruct(own.shape, BF16),
            jax.ShapeDtypeStruct(own.shape, BF16),
            jax.ShapeDtypeStruct(own.shape, BF16),
            jax.ShapeDtypeStruct((members, 4 * width // members, width), F32),
        ],
        name="forward",
    )(src, picks, place, tiles, own, near, far, degree, cot, w_self, w_neigh, *stale)


def backward_kernel(
    src_ref, tiles_ref, back_ref, halo_ref, own_ref, tiles, backs, even, odd, halos,
    tile_sems, in_sem, out_sems, *, group,
):
    blocks, width, tile = back_ref.shape
    tiles_row = src_ref.shape[0]
    halo = halo_ref.shape[0]

    def tile_copy(b):
        at = pl.ds(b * tiles_row, tiles_row)
        return pltpu.make_async_copy(tiles_ref.at[at], tiles.at[at], tile_sems.at[b])

    back_in = pltpu.make_async_copy(back_ref, backs, in_sem)
    back_in.start()

    @pl.loop(0, blocks)
    def _(b):
        tile_copy(b).start()

    @pl.loop(0, even.shape[0])
    def _(s):
        even[s] = jnp.zeros((width, tile), F32)
        odd[s] = jnp.zeros((width, tile), F32)

    back_in.wait()

    @pl.loop(0, blocks, step=group)
    def _(first):
        for k in range(group):
            tile_copy(first + k).wait()
        for k in range(group):
            b = first + k
            back = backs[b]
            for t in range(0, tiles_row, 2):
                at = b * tiles_row + t
                pair = jnp.concatenate([tiles[at], tiles[at + 1]], axis=1)
                got = jnp.dot(back, pair, preferred_element_type=F32)
                even[src_ref[t, b]] += got[:, :tile]
                odd[src_ref[t + 1, b]] += got[:, tile:]

    @pl.loop(0, halo, step=4)
    def _(s):
        for k in range(4):
            halos[s + k] = (even[blocks + s + k] + odd[blocks + s + k]).astype(BF16)

    halo_out = pltpu.make_async_copy(halos, halo_ref, out_sems.at[0])
    halo_out.start()

    @pl.loop(0, blocks, step=4)
    def _(s):
        for k in range(4):
            even[s + k] += odd[s + k]

    own_out = pltpu.make_async_copy(even.at[pl.ds(0, blocks)], own_ref, out_sems.at[1])
    own_out.start()
    halo_out.wait()
    own_out.wait()


def backward(src, tiles, back_t, halo, count, group=4):
    blocks, width, tile = back_t.shape
    grads = jax.ShapeDtypeStruct((blocks, width, tile), F32)
    return pl.pallas_call(
        functools.partial(backward_kernel, group=group),
        in_specs=[pl.BlockSpec(memory_space=pltpu.SMEM), any_spec(), any_spec()],
        out_specs=[any_spec()] * 2,
        scratch_shapes=[
            pltpu.VMEM(tiles.shape, BF16),
            pltpu.VMEM(back_t.shape, BF16),
            pltpu.VMEM((count, width, tile), F32),
            pltpu.VMEM((count, width, tile), F32),
            pltpu.VMEM((halo, width, tile), BF16),
            pltpu.SemaphoreType.DMA((blocks,)),
            pltpu.SemaphoreType.DMA,
            pltpu.SemaphoreType.DMA((2,)),
        ],
        out_shape=[jax.ShapeDtypeStruct((halo, width, tile), BF16), grads],
        name="backward",
    )(src, tiles, back_t)


def local_kernel(acc_ref, dpre_ref, w_ref, share_ref, out_ref, copies_ref):
    blocks, width, tile = acc_ref.shape
    for p in range(copies_ref.shape[0]):
        copies_ref[p] = share_ref[...]

    @pl.loop(0, blocks, step=4)
    def _(first):
        for k in range(4):
            b = first + k
            both = acc_ref[b] + jnp.dot(w_ref[...], dpre_ref[b], preferred_element_type=F32)
            out_ref[pl.ds(b * tile, tile), :] = both.T


def local_rows(acc, dpre_t, w_self, share, members):
    blocks, width, tile = acc.shape
    return pl.pallas_call(
        local_kernel,
        out_shape=[
            jax.ShapeDtypeStruct((blocks * tile, width), F32),
            jax.ShapeDtypeStruct((members, *share.shape), F32),
        ],
        name="local_rows",
    )(acc, dpre_t, w_self, share)


def final_kernel(
    parts_ref, returned_ref, rows_ref, local_ref, out_ref, spread, outs, sems, *, offered, chunk
):
    nodes, width = local_ref.shape
    members, _, tile = returned_ref.shape
    each = parts_ref.shape[1] // 2
    sums = [jnp.zeros((width, tile), F32) for _ in range(offered)]
    for p in range(members):
        block = returned_ref[p].astype(F32)
        wanted = parts_ref[p, each : each + 1, :]
        for k in range(offered):
            sums[k] += jnp.where(wanted == F32(k), block, F32(0))
    grad = jnp.concatenate([s.T for s in sums], axis=0)
    high = grad.astype(BF16)
    spread[:, :width] = high
    spread[:, width:] = (grad - high.astype(F32)).astype(BF16)
    copies = []
    for c in range(nodes // chunk):
        at = lax.broadcasted_iota(jnp.int32, (chunk, offered * tile), 0) + c * chunk
        hot = jnp.where(at == rows_ref[...], F32(1), F32(0)).astype(BF16)
        more = jnp.dot(hot, spread[...], preferred_element_type=F32)
        rows = slice(c * chunk, (c + 1) * chunk)
        outs[rows, :] = (local_ref[rows, :] + (more[:, :width] + more[:, width:])).astype(BF16)
        at = pl.ds(c * chunk, chunk)
        copies.append(pltpu.make_async_copy(outs.at[at], out_ref.at[at], sems.at[c]))
        copies[-1].start()
    for c in copies:
        c.wait()


def final(parts, returned, rows, local, offered, chunk=512):
    nodes, width = local.shape
    tile = returned.shape[2]
    return pl.pallas_call(
        functools.partial(final_kernel, offered=offered, chunk=chunk),
        out_specs=any_spec(),
        out_shape=jax.ShapeDtypeStruct((nodes, width), BF16),
        scratch_shapes=[
            pltpu.VMEM((offered * tile, 2 * width), BF16),
            pltpu.VMEM((nodes, width), BF16),
            pltpu.SemaphoreType.DMA((nodes // chunk,)),
        ],
        name="final",
    )(parts, returned, rows, local)


def on_device(
    features,
    history,
    tiles,
    tile_src,
    degree,
    boundary_rows,
    picks,
    stale_rows,
    w_self,
    w_neigh,
    cotangent,
):
    members = lax.axis_size("member")
    groups = lax.axis_size("group")
    tile = tiles.shape[1]
    width = features.shape[1]
    blocks = features.shape[0] // tile
    offered = boundary_rows.shape[1] // tile
    src = tile_src.T
    halves = bound_halves(boundary_rows, features, members, tile)
    near = exchange(halves, "member")
    place = jnp.stack([lax.axis_index("member") % 2, lax.axis_index("group")]).astype(jnp.int32)
    stale_rows, halves = lax.optimization_barrier((stale_rows, halves))
    stale = list(stale_rows_sent(place, stale_rows, history))
    for k in range(1, groups):
        stale[k] = lax.ppermute(stale[k], "group", [(g, (g + k) % groups) for g in range(groups)])
    near, *stale = lax.optimization_barrier((near, *stale))
    far = lax.ppermute(near, "member", [(m, m ^ 1) for m in range(members)])
    stale = [piece.reshape(-1, tile, width) for piece in stale]
    own = features.reshape(blocks, tile, width)
    out, dpre_t, back_t, part = forward(
        src,
        picks.reshape(1, -1),
        place,
        tiles,
        own,
        near,
        far,
        stale,
        degree.reshape(blocks, tile),
        cotangent.reshape(blocks, tile, width),
        w_self,
        w_neigh,
    )
    parts = exchange(part, "member")
    count = blocks + members + groups * stale[0].shape[0]
    halo_grad, own_grad = backward(src, tiles, back_t, members, count)
    parts, halo_grad, own_grad = lax.optimization_barrier((parts, halo_grad, own_grad))
    returned = exchange(halo_grad, "member")
    factor = 1.0 / math.sqrt(features.shape[0] * members * groups)
    share = parts[:, : parts.shape[1] // 2].sum(axis=0) * factor
    hop = 1
    while hop < groups:
        share += lax.ppermute(share, "group", [(g, g ^ hop) for g in range(groups)])
        hop *= 2
    local, copies = local_rows(own_grad, dpre_t, w_self, share, members)
    returned, copies, local = lax.optimization_barrier((returned, copies, local))
    full = exchange(copies, "member").reshape(-1, width)
    grad_features = final(parts, returned, boundary_rows, local, offered)
    grad_self, grad_neigh = full[:width], full[width:]
    return (out.reshape(-1, width), grad_features, grad_self, grad_neigh)


def solution(mesh):
    placed = (
        P(("group", "member"), None),
        P(("group", "member"), None),
        P(("group", "member"), None, None),
        P(("group", "member"), None),
        P(("group", "member")),
        P(("group", "member"), None),
        P(("group", "member"), None),
        P(("group", "member"), None),
        P(),
        P(),
        P(("group", "member"), None),
    )
    return jax.shard_map(
        on_device,
        mesh=mesh,
        in_specs=placed,
        out_specs=(P(("group", "member"), None), P(("group", "member"), None), P(), P()),
        check_vma=False,
    )
```

```python
import functools
import math

import jax
import jax.numpy as jnp
from jax import lax
from jax.experimental import pallas as pl
from jax.experimental.pallas import tpu as pltpu
from jax.sharding import PartitionSpec as P

F32 = jnp.float32
BF16 = jnp.bfloat16
MIB = 1024 * 1024


def exchange(value, axis):
    return lax.all_to_all(value, axis, split_axis=0, concat_axis=0, tiled=True)


def any_spec():
    return pl.BlockSpec(memory_space=pl.ANY)


def column(row, lanes):
    return jnp.broadcast_to(row, (lanes, lanes)).T


def picked_rows(rows, table_ref):
    nodes, lanes = table_ref.shape
    wide = 256
    col = jnp.concatenate([column(r, lanes) for r in rows], axis=0)
    off = col - lax.broadcasted_iota(jnp.int32, col.shape, 1)
    acc = jnp.zeros(col.shape, F32)
    for c in range(nodes // wide):
        hot = jnp.concatenate(
            [
                jnp.where(off == c * wide + k * lanes, F32(1), F32(0)).astype(BF16)
                for k in range(wide // lanes)
            ],
            axis=1,
        )
        acc += jnp.dot(hot, table_ref[c * wide : (c + 1) * wide, :], preferred_element_type=F32)
    return acc.astype(BF16)


def bound_kernel(rows_ref, table_ref, out_ref, halves, sems, *, tile):
    offered = rows_ref.shape[1] // tile
    got = picked_rows([rows_ref[:, k * tile : (k + 1) * tile] for k in range(offered)], table_ref)
    half = tile // 2
    for c in range(2):
        for k in range(offered):
            halves[c, k] = got[k * tile + c * half : k * tile + (c + 1) * half]
    copies = [
        pltpu.make_async_copy(halves.at[p % 2], out_ref.at[p], sems.at[p])
        for p in range(out_ref.shape[0])
    ]
    for c in copies:
        c.start()
    for c in copies:
        c.wait()


def bound_halves(rows, table, members, tile):
    offered = rows.shape[1] // tile
    width = table.shape[1]
    return pl.pallas_call(
        functools.partial(bound_kernel, tile=tile),
        out_specs=any_spec(),
        out_shape=jax.ShapeDtypeStruct((members, offered, tile // 2, width), BF16),
        scratch_shapes=[
            pltpu.VMEM((2, offered, tile // 2, width), BF16),
            pltpu.SemaphoreType.DMA((members,)),
        ],
        name="bound_halves",
    )(rows, table)


def stale_kernel(rows_ref, table_ref, *out_refs):
    lanes = table_ref.shape[1]
    count = rows_ref.shape[1] // lanes
    groups = len(out_refs)
    here = lax.axis_index("group")
    for k in range(groups):
        g = lax.rem(here + k, groups)
        rows = rows_ref[pl.ds(g, 1), :]
        out_refs[k][...] = picked_rows(
            [rows[:, c * lanes : (c + 1) * lanes] for c in range(count)], table_ref
        )


def stale_rows_sent(rows, table):
    groups, count = rows.shape
    vmem = pl.BlockSpec(memory_space=pltpu.VMEM)
    piece = jax.ShapeDtypeStruct((count, table.shape[1]), BF16)
    return pl.pallas_call(
        stale_kernel,
        in_specs=[vmem, vmem],
        out_specs=[vmem] * groups,
        out_shape=[piece] * groups,
        compiler_params=pltpu.CompilerParams(vmem_limit_bytes=12 * MIB),
        name="stale_rows_sent",
    )(rows, table)


def forward_kernel(
    src_ref, picks_ref, tiles_ref, own_ref, near_ref, far_ref, deg_ref, cot_ref, ws_ref,
    wn_ref, *refs, group, groups,
):
    stale_refs, refs = refs[:groups], refs[groups:]
    out_ref, dpre_t_ref, back_t_ref, part_out, *refs = refs
    tiles, sources, cots, aggs, outs, dpre_ts, back_ts, w_cat, inv, part_acc, *refs = refs
    part_ref, tile_sems, in_sems, out_sems, part_sem = refs
    blocks, tile, width = own_ref.shape
    tiles_row = src_ref.shape[0]
    members, offered, half, _ = near_ref.shape
    halo = members * offered
    stale = stale_refs[0].shape[0]
    core = lax.rem(lax.axis_index("member"), 2)
    here = lax.axis_index("group")

    def tile_copy(b):
        at = pl.ds(b * tiles_row, tiles_row)
        return pltpu.make_async_copy(tiles_ref.at[at], tiles.at[at], tile_sems.at[b])

    def halo_rows(which):
        return sources.at[pl.ds(blocks, halo), pl.ds(pl.multiple_of(which * half, half), half)]

    ins = [
        pltpu.make_async_copy(own_ref, sources.at[pl.ds(0, blocks)], in_sems.at[0]),
        pltpu.make_async_copy(near_ref.reshape(halo, half, width), halo_rows(core), in_sems.at[1]),
        pltpu.make_async_copy(far_ref.reshape(halo, half, width), halo_rows(1 - core), in_sems.at[2]),
        *[
            pltpu.make_async_copy(
                ref, sources.at[pl.ds(blocks + halo + k * stale, stale)], in_sems.at[3 + k]
            )
            for k, ref in enumerate(stale_refs)
        ],
    ]
    cot_in = pltpu.make_async_copy(cot_ref, cots, in_sems.at[3 + groups])
    for c in ins:
        c.start()
    tile_copy(0).start()
    cot_in.start()

    @pl.loop(1, blocks)
    def _(b):
        tile_copy(b).start()

    w_cat[:width, :] = ws_ref[...]
    w_cat[width:, :] = wn_ref[...]
    inv[...] = 1.0 / deg_ref[...].astype(F32)
    part_acc[...] = jnp.zeros_like(part_acc)
    for c in ins:
        c.wait()

    def source_of(b, t):
        s = src_ref[t, b]
        m = jnp.clip(s - blocks, 0, members - 1)
        near = blocks + m * offered + picks_ref[0, m]
        late = jnp.maximum(s - blocks - members, 0)
        from_group = late // stale
        back = here - from_group
        back = jnp.where(back < 0, back + groups, back)
        old = blocks + halo + back * stale + late - from_group * stale
        return jnp.where(s < blocks, s, jnp.where(s < blocks + members, near, old))

    outputs = ((outs, out_ref), (dpre_ts, dpre_t_ref), (back_ts, back_t_ref))

    def out_copies(g):
        at = pl.ds(g * group, group)
        return [
            pltpu.make_async_copy(buf.at[at], ref.at[at], out_sems.at[k, g])
            for k, (buf, ref) in enumerate(outputs)
        ]

    def arrived(g):
        for k in range(group):
            tile_copy(g * group + k).wait()

    def aggregate(g):
        for k in range(group):
            b = g * group + k
            lhs = jnp.concatenate(
                [tiles[b * tiles_row + t] for t in range(tiles_row)], axis=1
            )
            rhs = jnp.concatenate([sources[source_of(b, t)] for t in range(tiles_row)], axis=0)
            summed = jnp.dot(lhs, rhs, preferred_element_type=F32)
            aggs[b] = (summed * column(inv[pl.ds(b, 1), :], tile)).astype(BF16)

    def dense(g):
        at = pl.ds(g * group, group)
        rows = group * tile
        x = jnp.concatenate(
            [sources[at].reshape(rows, width), aggs[at].reshape(rows, width)], axis=1
        )
        pre = jnp.dot(x, w_cat[...], preferred_element_type=F32)
        scale = lax.rsqrt(jnp.mean(pre * pre, axis=-1, keepdims=True) + 1e-05)
        outs[at] = (pre * scale).astype(BF16).reshape(group, tile, width)
        grad = cots[at].reshape(rows, width).astype(F32)
        mix = jnp.mean(grad * pre, axis=-1, keepdims=True)
        dpre = (scale * grad - pre * (scale * scale * scale * mix)).astype(BF16)
        dpre_t = jnp.concatenate(
            [dpre[k * tile : (k + 1) * tile].T for k in range(group)], axis=1
        )
        inv_row = jnp.concatenate([inv[pl.ds(g * group + k, 1), :] for k in range(group)], axis=1)
        back = jnp.dot(wn_ref[...], dpre_t, preferred_element_type=F32) * inv_row
        part_acc[...] += jnp.dot(dpre_t, x, preferred_element_type=F32)
        for k in range(group):
            dpre_ts[g * group + k] = dpre_t[:, k * tile : (k + 1) * tile]
            back_ts[g * group + k] = back[:, k * tile : (k + 1) * tile].astype(BF16)

    last = blocks // group - 1
    arrived(0)
    aggregate(0)
    cot_in.wait()

    @pl.loop(1, last + 1)
    def _(g):
        arrived(g)
        dense(g - 1)
        aggregate(g)
        for c in out_copies(g - 1):
            c.start()

    dense(last)
    for c in out_copies(last):
        c.start()

    each = 2 * width // members
    for q in range(2):
        grad = part_acc[:, q * width : (q + 1) * width].T
        for p in range(members // 2):
            part_ref[q * (members // 2) + p, :each] = grad[p * each : (p + 1) * each]
    for p in range(members):
        part_ref[p, each:] = jnp.full((each, width), picks_ref[0, p].astype(F32), F32)
    part_copy = pltpu.make_async_copy(part_ref, part_out, part_sem)
    part_copy.start()

    @pl.loop(0, blocks // group)
    def _(g):
        for c in out_copies(g):
            c.wait()

    part_copy.wait()


def forward(src, picks, tiles, own, near, far, stale, degree, cot, w_self, w_neigh, group=4):
    blocks, tile, width = own.shape
    members, offered = near.shape[:2]
    groups = len(stale)
    count = blocks + members * offered + groups * stale[0].shape[0]
    smem = pl.BlockSpec(memory_space=pltpu.SMEM)
    vmem = pl.BlockSpec(memory_space=pltpu.VMEM)
    node = pltpu.VMEM((blocks, tile, width), BF16)
    return pl.pallas_call(
        functools.partial(forward_kernel, group=group, groups=groups),
        in_specs=[smem] * 2 + [any_spec()] * 4 + [vmem, any_spec(), vmem, vmem] + [any_spec()] * groups,
        out_specs=[any_spec()] * 4,
        scratch_shapes=[
            pltpu.VMEM(tiles.shape, BF16),
            pltpu.VMEM((count, tile, width), BF16),
            node,
            node,
            node,
            node,
            node,
            pltpu.VMEM((2 * width, width), BF16),
            pltpu.VMEM((blocks, tile), F32),
            pltpu.VMEM((width, 2 * width), F32),
            pltpu.VMEM((members, 4 * width // members, width), F32),
            pltpu.SemaphoreType.DMA((blocks,)),
            pltpu.SemaphoreType.DMA((4 + groups,)),
            pltpu.SemaphoreType.DMA((3, blocks // group)),
            pltpu.SemaphoreType.DMA,
        ],
        out_shape=[
            pltpu.HBM(own.shape, BF16),
            pltpu.HBM(own.shape, BF16),
            pltpu.HBM(own.shape, BF16),
            pltpu.HBM((members, 4 * width // members, width), F32),
        ],
        compiler_params=pltpu.CompilerParams(vmem_limit_bytes=40 * MIB),
        name="forward",
    )(src, picks, tiles, own, near, far, degree, cot, w_self, w_neigh, *stale)


def backward_kernel(
    src_ref, tiles_ref, back_ref, halo_ref, own_ref, tiles, backs, even, odd, halos,
    tile_sems, in_sem, out_sems, *, group,
):
    blocks, width, tile = back_ref.shape
    tiles_row = src_ref.shape[0]
    halo = halo_ref.shape[0]

    def tile_copy(b):
        at = pl.ds(b * tiles_row, tiles_row)
        return pltpu.make_async_copy(tiles_ref.at[at], tiles.at[at], tile_sems.at[b])

    back_in = pltpu.make_async_copy(back_ref, backs, in_sem)
    back_in.start()

    @pl.loop(0, blocks)
    def _(b):
        tile_copy(b).start()

    @pl.loop(0, even.shape[0])
    def _(s):
        even[s] = jnp.zeros((width, tile), F32)
        odd[s] = jnp.zeros((width, tile), F32)

    back_in.wait()

    @pl.loop(0, blocks, step=group)
    def _(first):
        for k in range(group):
            tile_copy(first + k).wait()
        for k in range(group):
            b = first + k
            back = backs[b]
            for t in range(0, tiles_row, 2):
                at = b * tiles_row + t
                pair = jnp.concatenate([tiles[at], tiles[at + 1]], axis=1)
                got = jnp.dot(back, pair, preferred_element_type=F32)
                even[src_ref[t, b]] += got[:, :tile]
                odd[src_ref[t + 1, b]] += got[:, tile:]

    @pl.loop(0, halo, step=4)
    def _(s):
        for k in range(4):
            halos[s + k] = (even[blocks + s + k] + odd[blocks + s + k]).astype(BF16)

    halo_out = pltpu.make_async_copy(halos, halo_ref, out_sems.at[0])
    halo_out.start()

    @pl.loop(0, blocks, step=4)
    def _(s):
        for k in range(4):
            even[s + k] += odd[s + k]

    own_out = pltpu.make_async_copy(even.at[pl.ds(0, blocks)], own_ref, out_sems.at[1])
    own_out.start()
    halo_out.wait()
    own_out.wait()


def backward(src, tiles, back_t, halo, count, group=4):
    blocks, width, tile = back_t.shape
    grads = pltpu.HBM((blocks, width, tile), F32)
    return pl.pallas_call(
        functools.partial(backward_kernel, group=group),
        in_specs=[pl.BlockSpec(memory_space=pltpu.SMEM), any_spec(), any_spec()],
        out_specs=[any_spec()] * 2,
        scratch_shapes=[
            pltpu.VMEM(tiles.shape, BF16),
            pltpu.VMEM(back_t.shape, BF16),
            pltpu.VMEM((count, width, tile), F32),
            pltpu.VMEM((count, width, tile), F32),
            pltpu.VMEM((halo, width, tile), BF16),
            pltpu.SemaphoreType.DMA((blocks,)),
            pltpu.SemaphoreType.DMA,
            pltpu.SemaphoreType.DMA((2,)),
        ],
        out_shape=[jax.ShapeDtypeStruct((halo, width, tile), BF16), grads],
        name="backward",
    )(src, tiles, back_t)


def local_kernel(acc_ref, dpre_ref, w_ref, share_ref, out_ref, copies_ref):
    blocks, width, tile = acc_ref.shape
    for p in range(copies_ref.shape[0]):
        copies_ref[p] = share_ref[...]

    @pl.loop(0, blocks, step=4)
    def _(first):
        for k in range(4):
            b = first + k
            both = acc_ref[b] + jnp.dot(w_ref[...], dpre_ref[b], preferred_element_type=F32)
            out_ref[pl.ds(b * tile, tile), :] = both.T


def local_rows(acc, dpre_t, w_self, share, members):
    blocks, width, tile = acc.shape
    return pl.pallas_call(
        local_kernel,
        out_shape=[
            jax.ShapeDtypeStruct((blocks * tile, width), F32),
            jax.ShapeDtypeStruct((members, *share.shape), F32),
        ],
        compiler_params=pltpu.CompilerParams(vmem_limit_bytes=12 * MIB),
        name="local_rows",
    )(acc, dpre_t, w_self, share)


def final_kernel(
    parts_ref, returned_ref, rows_ref, local_ref, out_ref, spread, outs, sems, *, offered, chunk
):
    nodes, width = local_ref.shape
    members, _, tile = returned_ref.shape
    each = parts_ref.shape[1] // 2
    sums = [jnp.zeros((width, tile), F32) for _ in range(offered)]
    for p in range(members):
        block = returned_ref[p].astype(F32)
        wanted = parts_ref[p, each : each + 1, :]
        for k in range(offered):
            sums[k] += jnp.where(wanted == F32(k), block, F32(0))
    grad = jnp.concatenate([s.T for s in sums], axis=0)
    high = grad.astype(BF16)
    spread[:, :width] = high
    spread[:, width:] = (grad - high.astype(F32)).astype(BF16)
    copies = []
    for c in range(nodes // chunk):
        at = lax.broadcasted_iota(jnp.int32, (chunk, offered * tile), 0) + c * chunk
        hot = jnp.where(at == rows_ref[...], F32(1), F32(0)).astype(BF16)
        more = jnp.dot(hot, spread[...], preferred_element_type=F32)
        rows = slice(c * chunk, (c + 1) * chunk)
        outs[rows, :] = (local_ref[rows, :] + (more[:, :width] + more[:, width:])).astype(BF16)
        at = pl.ds(c * chunk, chunk)
        copies.append(pltpu.make_async_copy(outs.at[at], out_ref.at[at], sems.at[c]))
        copies[-1].start()
    for c in copies:
        c.wait()


def final(parts, returned, rows, local, offered, chunk=512):
    nodes, width = local.shape
    tile = returned.shape[2]
    return pl.pallas_call(
        functools.partial(final_kernel, offered=offered, chunk=chunk),
        out_specs=any_spec(),
        out_shape=jax.ShapeDtypeStruct((nodes, width), BF16),
        scratch_shapes=[
            pltpu.VMEM((offered * tile, 2 * width), BF16),
            pltpu.VMEM((nodes, width), BF16),
            pltpu.SemaphoreType.DMA((nodes // chunk,)),
        ],
        compiler_params=pltpu.CompilerParams(vmem_limit_bytes=12 * MIB),
        name="final",
    )(parts, returned, rows, local)


def on_device(
    features,
    history,
    tiles,
    tile_src,
    degree,
    boundary_rows,
    picks,
    stale_rows,
    w_self,
    w_neigh,
    cotangent,
):
    members = lax.axis_size("member")
    groups = lax.axis_size("group")
    tile = tiles.shape[1]
    width = features.shape[1]
    blocks = features.shape[0] // tile
    offered = boundary_rows.shape[1] // tile
    src = tile_src.T
    halves = bound_halves(boundary_rows, features, members, tile)
    near = exchange(halves, "member")
    stale_rows, halves = lax.optimization_barrier((stale_rows, halves))
    stale = list(stale_rows_sent(stale_rows, history))
    for k in range(1, groups):
        stale[k] = lax.ppermute(stale[k], "group", [(g, (g + k) % groups) for g in range(groups)])
    near, *stale = lax.optimization_barrier((near, *stale))
    far = lax.ppermute(near, "member", [(m, m ^ 1) for m in range(members)])
    stale = [piece.reshape(-1, tile, width) for piece in stale]
    own = features.reshape(blocks, tile, width)
    tiles = pltpu.with_memory_space_constraint(tiles, pltpu.HBM)
    out, dpre_t, back_t, part = forward(
        src,
        picks.reshape(1, -1),
        tiles,
        own,
        near,
        far,
        stale,
        degree.reshape(blocks, tile),
        cotangent.reshape(blocks, tile, width),
        w_self,
        w_neigh,
    )
    parts = exchange(part, "member")
    count = blocks + members + groups * stale[0].shape[0]
    halo_grad, own_grad = backward(src, tiles, back_t, members, count)
    parts, halo_grad, own_grad = lax.optimization_barrier((parts, halo_grad, own_grad))
    returned = exchange(halo_grad, "member")
    factor = 1.0 / math.sqrt(features.shape[0] * members * groups)
    share = parts[:, : parts.shape[1] // 2].sum(axis=0) * factor
    hop = 1
    while hop < groups:
        share += lax.ppermute(share, "group", [(g, g ^ hop) for g in range(groups)])
        hop *= 2
    local, copies = local_rows(own_grad, dpre_t, w_self, share, members)
    returned, copies, local = lax.optimization_barrier((returned, copies, local))
    full = exchange(copies, "member").reshape(-1, width)
    grad_features = final(parts, returned, boundary_rows, local, offered)
    grad_self, grad_neigh = full[:width], full[width:]
    return (out.reshape(-1, width), grad_features, grad_self, grad_neigh)


def solution(mesh):
    placed = (
        P(("group", "member"), None),
        P(("group", "member"), None),
        P(("group", "member"), None, None),
        P(("group", "member"), None),
        P(("group", "member")),
        P(("group", "member"), None),
        P(("group", "member"), None),
        P(("group", "member"), None),
        P(),
        P(),
        P(("group", "member"), None),
    )
    return jax.shard_map(
        on_device,
        mesh=mesh,
        in_specs=placed,
        out_specs=(P(("group", "member"), None), P(("group", "member"), None), P(), P()),
        check_vma=False,
    )
```

```python
import functools
import math

import jax
import jax.numpy as jnp
from jax import lax
from jax.experimental import pallas as pl
from jax.experimental.pallas import tpu as pltpu
from jax.sharding import PartitionSpec as P


F32 = jnp.float32
BF16 = jnp.bfloat16
MIB = 1024 * 1024


def exchange(value, axis):
    return lax.all_to_all(value, axis, split_axis=0, concat_axis=0, tiled=True)


def partner(value, axis, mask):
    size = lax.axis_size(axis)
    return lax.ppermute(value, axis, [(m, m ^ mask) for m in range(size)])


def any_spec():
    return pl.BlockSpec(memory_space=pl.ANY)


def column(row, lanes):
    return jnp.broadcast_to(row, (lanes, lanes)).T


def picked_rows(rows, table_ref):
    nodes, lanes = table_ref.shape
    wide = 256
    col = jnp.concatenate([column(r, lanes) for r in rows], axis=0)
    off = col - lax.broadcasted_iota(jnp.int32, col.shape, 1)
    acc = jnp.zeros(col.shape, F32)
    for c in range(nodes // wide):
        hot = jnp.concatenate(
            [
                jnp.where(off == c * wide + k * lanes, F32(1), F32(0)).astype(BF16)
                for k in range(wide // lanes)
            ],
            axis=1,
        )
        acc += jnp.dot(hot, table_ref[c * wide : (c + 1) * wide, :], preferred_element_type=F32)
    return acc.astype(BF16)


def bound_kernel(rows_ref, table_ref, out_ref, halves, sems, *, tile):
    offered = rows_ref.shape[1] // tile
    got = picked_rows([rows_ref[:, k * tile : (k + 1) * tile] for k in range(offered)], table_ref)
    half = tile // 2
    for c in range(2):
        for k in range(offered):
            halves[c, k] = got[k * tile + c * half : k * tile + (c + 1) * half]
    copies = [
        pltpu.make_async_copy(halves.at[p % 2], out_ref.at[p], sems.at[p])
        for p in range(out_ref.shape[0])
    ]
    for c in copies:
        c.start()
    for c in copies:
        c.wait()


def bound_halves(rows, table, members, tile):
    offered = rows.shape[1] // tile
    width = table.shape[1]
    return pl.pallas_call(
        functools.partial(bound_kernel, tile=tile),
        out_specs=any_spec(),
        out_shape=jax.ShapeDtypeStruct((members, offered, tile // 2, width), BF16),
        scratch_shapes=[
            pltpu.VMEM((2, offered, tile // 2, width), BF16),
            pltpu.SemaphoreType.DMA((members,)),
        ],
        name="bound_halves",
    )(rows, table)


def stale_kernel(rows_ref, table_ref, *out_refs):
    lanes = table_ref.shape[1]
    count = rows_ref.shape[1] // lanes
    groups = len(out_refs)
    here = lax.axis_index("group")
    for k in range(groups):
        g = lax.rem(here + k, groups)
        rows = rows_ref[pl.ds(g, 1), :]
        out_refs[k][...] = picked_rows(
            [rows[:, c * lanes : (c + 1) * lanes] for c in range(count)], table_ref
        )


def stale_rows_sent(rows, table):
    groups, count = rows.shape
    vmem = pl.BlockSpec(memory_space=pltpu.VMEM)
    piece = jax.ShapeDtypeStruct((count, table.shape[1]), BF16)
    return pl.pallas_call(
        stale_kernel,
        in_specs=[vmem, vmem],
        out_specs=[vmem] * groups,
        out_shape=[piece] * groups,
        compiler_params=pltpu.CompilerParams(vmem_limit_bytes=12 * MIB),
        name="stale_rows_sent",
    )(rows, table)


def forward_kernel(
    src_ref, picks_ref, tiles_ref, own_ref, near_ref, far_ref, deg_ref, cot_ref, ws_ref,
    wn_ref, *refs, group, groups,
):
    stale_refs, refs = refs[:groups], refs[groups:]
    out_ref, dpre_t_ref, back_t_ref, part_out, *refs = refs
    tiles, sources, cots, aggs, outs, dpre_ts, back_ts, w_cat, inv, part_acc, *refs = refs
    part_ref, tile_sems, in_sems, out_sems, part_sem = refs
    blocks, tile, width = own_ref.shape
    tiles_row = src_ref.shape[0]
    members, offered, half, _ = near_ref.shape
    halo = members * offered
    stale = stale_refs[0].shape[0]
    core = lax.rem(lax.axis_index("member"), 2)
    here = lax.axis_index("group")

    def tile_copy(b):
        at = pl.ds(b * tiles_row, tiles_row)
        return pltpu.make_async_copy(tiles_ref.at[at], tiles.at[at], tile_sems.at[b])

    def halo_rows(which):
        return sources.at[pl.ds(blocks, halo), pl.ds(pl.multiple_of(which * half, half), half)]

    ins = [
        pltpu.make_async_copy(own_ref, sources.at[pl.ds(0, blocks)], in_sems.at[0]),
        pltpu.make_async_copy(near_ref.reshape(halo, half, width), halo_rows(core), in_sems.at[1]),
        pltpu.make_async_copy(far_ref.reshape(halo, half, width), halo_rows(1 - core), in_sems.at[2]),
        *[
            pltpu.make_async_copy(
                ref, sources.at[pl.ds(blocks + halo + k * stale, stale)], in_sems.at[3 + k]
            )
            for k, ref in enumerate(stale_refs)
        ],
    ]
    cot_in = pltpu.make_async_copy(cot_ref, cots, in_sems.at[3 + groups])
    for c in ins:
        c.start()
    tile_copy(0).start()
    cot_in.start()

    @pl.loop(1, blocks)
    def _(b):
        tile_copy(b).start()

    w_cat[:width, :] = ws_ref[...]
    w_cat[width:, :] = wn_ref[...]
    inv[...] = 1.0 / deg_ref[...].astype(F32)
    part_acc[...] = jnp.zeros_like(part_acc)
    for c in ins:
        c.wait()

    def source_of(b, t):
        s = src_ref[t, b]
        m = jnp.clip(s - blocks, 0, members - 1)
        near = blocks + m * offered + picks_ref[0, m]
        late = jnp.maximum(s - blocks - members, 0)
        from_group = late // stale
        back = here - from_group
        back = jnp.where(back < 0, back + groups, back)
        old = blocks + halo + back * stale + late - from_group * stale
        return jnp.where(s < blocks, s, jnp.where(s < blocks + members, near, old))

    outputs = ((outs, out_ref), (dpre_ts, dpre_t_ref), (back_ts, back_t_ref))

    def out_copies(g):
        at = pl.ds(g * group, group)
        return [
            pltpu.make_async_copy(buf.at[at], ref.at[at], out_sems.at[k, g])
            for k, (buf, ref) in enumerate(outputs)
        ]

    def arrived(g):
        for k in range(group):
            tile_copy(g * group + k).wait()

    def aggregate(g):
        for k in range(group):
            b = g * group + k
            lhs = jnp.concatenate(
                [tiles[b * tiles_row + t] for t in range(tiles_row)], axis=1
            )
            rhs = jnp.concatenate([sources[source_of(b, t)] for t in range(tiles_row)], axis=0)
            summed = jnp.dot(lhs, rhs, preferred_element_type=F32)
            aggs[b] = (summed * column(inv[pl.ds(b, 1), :], tile)).astype(BF16)

    def dense(g):
        at = pl.ds(g * group, group)
        rows = group * tile
        x = jnp.concatenate(
            [sources[at].reshape(rows, width), aggs[at].reshape(rows, width)], axis=1
        )
        pre = jnp.dot(x, w_cat[...], preferred_element_type=F32)
        scale = lax.rsqrt(jnp.mean(pre * pre, axis=-1, keepdims=True) + 1e-05)
        outs[at] = (pre * scale).astype(BF16).reshape(group, tile, width)
        grad = cots[at].reshape(rows, width).astype(F32)
        mix = jnp.mean(grad * pre, axis=-1, keepdims=True)
        dpre = (scale * grad - pre * (scale * scale * scale * mix)).astype(BF16)
        dpre_t = jnp.concatenate(
            [dpre[k * tile : (k + 1) * tile].T for k in range(group)], axis=1
        )
        inv_row = jnp.concatenate([inv[pl.ds(g * group + k, 1), :] for k in range(group)], axis=1)
        back = jnp.dot(wn_ref[...], dpre_t, preferred_element_type=F32) * inv_row
        part_acc[...] += jnp.dot(dpre_t, x, preferred_element_type=F32)
        for k in range(group):
            dpre_ts[g * group + k] = dpre_t[:, k * tile : (k + 1) * tile]
            back_ts[g * group + k] = back[:, k * tile : (k + 1) * tile].astype(BF16)

    last = blocks // group - 1
    arrived(0)
    aggregate(0)
    cot_in.wait()

    @pl.loop(1, last + 1)
    def _(g):
        arrived(g)
        dense(g - 1)
        aggregate(g)
        for c in out_copies(g - 1):
            c.start()

    dense(last)
    for c in out_copies(last):
        c.start()

    each = 2 * width // members
    for q in range(2):
        grad = part_acc[:, q * width : (q + 1) * width].T
        for p in range(members // 2):
            part_ref[q * (members // 2) + p, :each] = grad[p * each : (p + 1) * each]
    for p in range(members):
        part_ref[p, each:] = jnp.full((each, width), picks_ref[0, p].astype(F32), F32)
    part_copy = pltpu.make_async_copy(part_ref, part_out, part_sem)
    part_copy.start()

    @pl.loop(0, blocks // group)
    def _(g):
        for c in out_copies(g):
            c.wait()

    part_copy.wait()


def forward(src, picks, tiles, own, near, far, stale, degree, cot, w_self, w_neigh, group=4):
    blocks, tile, width = own.shape
    members, offered = near.shape[:2]
    groups = len(stale)
    count = blocks + members * offered + groups * stale[0].shape[0]
    smem = pl.BlockSpec(memory_space=pltpu.SMEM)
    vmem = pl.BlockSpec(memory_space=pltpu.VMEM)
    node = pltpu.VMEM((blocks, tile, width), BF16)
    return pl.pallas_call(
        functools.partial(forward_kernel, group=group, groups=groups),
        in_specs=[smem] * 2 + [any_spec()] * 4 + [vmem, any_spec(), vmem, vmem] + [any_spec()] * groups,
        out_specs=[any_spec()] * 4,
        scratch_shapes=[
            pltpu.VMEM(tiles.shape, BF16),
            pltpu.VMEM((count, tile, width), BF16),
            node,
            node,
            node,
            node,
            node,
            pltpu.VMEM((2 * width, width), BF16),
            pltpu.VMEM((blocks, tile), F32),
            pltpu.VMEM((width, 2 * width), F32),
            pltpu.VMEM((members, 4 * width // members, width), F32),
            pltpu.SemaphoreType.DMA((blocks,)),
            pltpu.SemaphoreType.DMA((4 + groups,)),
            pltpu.SemaphoreType.DMA((3, blocks // group)),
            pltpu.SemaphoreType.DMA,
        ],
        out_shape=[
            pltpu.HBM(own.shape, BF16),
            pltpu.HBM(own.shape, BF16),
            pltpu.HBM(own.shape, BF16),
            pltpu.HBM((members, 4 * width // members, width), F32),
        ],
        compiler_params=pltpu.CompilerParams(vmem_limit_bytes=40 * MIB),
        name="forward",
    )(src, picks, tiles, own, near, far, degree, cot, w_self, w_neigh, *stale)


def backward_kernel(
    src_ref, tiles_ref, back_ref, halo_ref, own_ref, tiles, backs, even, odd, halos,
    tile_sems, in_sem, out_sems, *, group,
):
    blocks, width, tile = back_ref.shape
    tiles_row = src_ref.shape[0]
    halo = halo_ref.shape[0]

    def tile_copy(b):
        at = pl.ds(b * tiles_row, tiles_row)
        return pltpu.make_async_copy(tiles_ref.at[at], tiles.at[at], tile_sems.at[b])

    back_in = pltpu.make_async_copy(back_ref, backs, in_sem)
    back_in.start()

    @pl.loop(0, blocks)
    def _(b):
        tile_copy(b).start()

    @pl.loop(0, even.shape[0])
    def _(s):
        even[s] = jnp.zeros((width, tile), F32)
        odd[s] = jnp.zeros((width, tile), F32)

    back_in.wait()

    @pl.loop(0, blocks, step=group)
    def _(first):
        for k in range(group):
            tile_copy(first + k).wait()
        for k in range(group):
            b = first + k
            back = backs[b]
            for t in range(0, tiles_row, 2):
                at = b * tiles_row + t
                pair = jnp.concatenate([tiles[at], tiles[at + 1]], axis=1)
                got = jnp.dot(back, pair, preferred_element_type=F32)
                even[src_ref[t, b]] += got[:, :tile]
                odd[src_ref[t + 1, b]] += got[:, tile:]

    @pl.loop(0, halo, step=4)
    def _(s):
        for k in range(4):
            halos[s + k] = (even[blocks + s + k] + odd[blocks + s + k]).astype(BF16)

    halo_out = pltpu.make_async_copy(halos, halo_ref, out_sems.at[0])
    halo_out.start()

    @pl.loop(0, blocks, step=4)
    def _(s):
        for k in range(4):
            even[s + k] += odd[s + k]

    own_out = pltpu.make_async_copy(even.at[pl.ds(0, blocks)], own_ref, out_sems.at[1])
    own_out.start()
    halo_out.wait()
    own_out.wait()


def backward(src, tiles, back_t, halo, count, group=4):
    blocks, width, tile = back_t.shape
    grads = pltpu.HBM((blocks, width, tile), F32)
    return pl.pallas_call(
        functools.partial(backward_kernel, group=group),
        in_specs=[pl.BlockSpec(memory_space=pltpu.SMEM), any_spec(), any_spec()],
        out_specs=[any_spec()] * 2,
        scratch_shapes=[
            pltpu.VMEM(tiles.shape, BF16),
            pltpu.VMEM(back_t.shape, BF16),
            pltpu.VMEM((count, width, tile), F32),
            pltpu.VMEM((count, width, tile), F32),
            pltpu.VMEM((halo, width, tile), BF16),
            pltpu.SemaphoreType.DMA((blocks,)),
            pltpu.SemaphoreType.DMA,
            pltpu.SemaphoreType.DMA((2,)),
        ],
        out_shape=[jax.ShapeDtypeStruct((halo, width, tile), BF16), grads],
        name="backward",
    )(src, tiles, back_t)


def local_kernel(acc_ref, dpre_ref, w_ref, out_ref):
    blocks, _, tile = acc_ref.shape

    @pl.loop(0, blocks, step=4)
    def _(first):
        for k in range(4):
            b = first + k
            both = acc_ref[b] + jnp.dot(w_ref[...], dpre_ref[b], preferred_element_type=F32)
            out_ref[pl.ds(b * tile, tile), :] = both.T


def local_rows(acc, dpre_t, w_self):
    blocks, width, tile = acc.shape
    return pl.pallas_call(
        local_kernel,
        out_shape=jax.ShapeDtypeStruct((blocks * tile, width), F32),
        compiler_params=pltpu.CompilerParams(vmem_limit_bytes=12 * MIB),
        name="local_rows",
    )(acc, dpre_t, w_self)


def final_kernel(
    parts_ref, returned_ref, rows_ref, local_ref, same_ref, other_ref,
    out_ref, self_ref, neigh_ref, spread, outs, sems, *, offered, chunk,
):
    nodes, width = local_ref.shape
    members, _, tile = returned_ref.shape
    each = parts_ref.shape[1] // 2
    sums = [jnp.zeros((width, tile), F32) for _ in range(offered)]
    for p in range(members):
        block = returned_ref[p].astype(F32)
        wanted = parts_ref[p, each : each + 1, :]
        for k in range(offered):
            sums[k] += jnp.where(wanted == F32(k), block, F32(0))
    grad = jnp.concatenate([s.T for s in sums], axis=0)
    high = grad.astype(BF16)
    spread[:, :width] = high
    spread[:, width:] = (grad - high.astype(F32)).astype(BF16)
    copies = []
    for c in range(nodes // chunk):
        at = lax.broadcasted_iota(jnp.int32, (chunk, offered * tile), 0) + c * chunk
        hot = jnp.where(at == rows_ref[...], F32(1), F32(0)).astype(BF16)
        more = jnp.dot(hot, spread[...], preferred_element_type=F32)
        rows = slice(c * chunk, (c + 1) * chunk)
        outs[rows, :] = (local_ref[rows, :] + (more[:, :width] + more[:, width:])).astype(BF16)
        at = pl.ds(c * chunk, chunk)
        copies.append(pltpu.make_async_copy(outs.at[at], out_ref.at[at], sems.at[c]))
        copies[-1].start()
    here = lax.axis_index("member")
    for p in range(members):
        apart = here ^ p
        at = apart // 2
        block = jnp.where(apart % 2 == 0, same_ref[at], other_ref[at])
        q, at = divmod(p * each, width)
        (self_ref, neigh_ref)[q][at : at + each, :] = block
    for c in copies:
        c.wait()


def final(parts, returned, rows, local, same, other, offered, chunk=512):
    nodes, width = local.shape
    tile = returned.shape[2]
    vmem = pl.BlockSpec(memory_space=pltpu.VMEM)
    square = jax.ShapeDtypeStruct((width, width), F32)
    return pl.pallas_call(
        functools.partial(final_kernel, offered=offered, chunk=chunk),
        out_specs=[any_spec(), vmem, vmem],
        out_shape=[jax.ShapeDtypeStruct((nodes, width), BF16), square, square],
        scratch_shapes=[
            pltpu.VMEM((offered * tile, 2 * width), BF16),
            pltpu.VMEM((nodes, width), BF16),
            pltpu.SemaphoreType.DMA((nodes // chunk,)),
        ],
        compiler_params=pltpu.CompilerParams(vmem_limit_bytes=12 * MIB),
        name="final",
    )(parts, returned, rows, local, same, other)


def on_device(
    features,
    history,
    tiles,
    tile_src,
    degree,
    boundary_rows,
    picks,
    stale_rows,
    w_self,
    w_neigh,
    cotangent,
):
    members = lax.axis_size("member")
    groups = lax.axis_size("group")
    tile = tiles.shape[1]
    width = features.shape[1]
    blocks = features.shape[0] // tile
    offered = boundary_rows.shape[1] // tile
    src = tile_src.T
    halves = bound_halves(boundary_rows, features, members, tile)
    near = exchange(halves, "member")
    stale_rows, halves = lax.optimization_barrier((stale_rows, halves))
    stale = list(stale_rows_sent(stale_rows, history))
    for k in range(1, groups):
        stale[k] = lax.ppermute(stale[k], "group", [(g, (g + k) % groups) for g in range(groups)])
    near, *stale = lax.optimization_barrier((near, *stale))
    far = lax.ppermute(near, "member", [(m, m ^ 1) for m in range(members)])
    stale = [piece.reshape(-1, tile, width) for piece in stale]
    own = features.reshape(blocks, tile, width)
    tiles = pltpu.with_memory_space_constraint(tiles, pltpu.HBM)
    out, dpre_t, back_t, part = forward(
        src,
        picks.reshape(1, -1),
        tiles,
        own,
        near,
        far,
        stale,
        degree.reshape(blocks, tile),
        cotangent.reshape(blocks, tile, width),
        w_self,
        w_neigh,
    )
    parts = exchange(part, "member")
    count = blocks + members + groups * stale[0].shape[0]
    halo_grad, own_grad = backward(src, tiles, back_t, members, count)
    parts, halo_grad, own_grad = lax.optimization_barrier((parts, halo_grad, own_grad))
    returned = exchange(halo_grad, "member")
    factor = 1.0 / math.sqrt(features.shape[0] * members * groups)
    share = parts[:, : parts.shape[1] // 2].sum(axis=0) * factor
    seen = [share] + [partner(share, "group", k) for k in range(1, groups)]
    while len(seen) > 1:
        seen = [a + b for a, b in zip(seen[::2], seen[1::2])]
    same = seen[0][None]
    side = math.isqrt(members // 2)
    for stride in (2, 2 * side):
        same = jnp.concatenate(
            [same] + [partner(same, "member", k * stride) for k in range(1, side)], axis=0
        )
    other = partner(same, "member", 1)
    local = local_rows(own_grad, dpre_t, w_self)
    grad_features, grad_self, grad_neigh = final(
        parts, returned, boundary_rows, local, same, other, offered
    )
    return (out.reshape(-1, width), grad_features, grad_self, grad_neigh)


def solution(mesh):
    placed = (
        P(("group", "member"), None),
        P(("group", "member"), None),
        P(("group", "member"), None, None),
        P(("group", "member"), None),
        P(("group", "member")),
        P(("group", "member"), None),
        P(("group", "member"), None),
        P(("group", "member"), None),
        P(),
        P(),
        P(("group", "member"), None),
    )
    return jax.shard_map(
        on_device,
        mesh=mesh,
        in_specs=placed,
        out_specs=(P(("group", "member"), None), P(("group", "member"), None), P(), P()),
        check_vma=False,
    )
```

```python
import functools
import math

import jax
import jax.numpy as jnp
from jax import lax
from jax.experimental import pallas as pl
from jax.experimental.pallas import tpu as pltpu
from jax.sharding import PartitionSpec as P


F32 = jnp.float32
BF16 = jnp.bfloat16
MIB = 1024 * 1024


def exchange(value, axis):
    return lax.all_to_all(value, axis, split_axis=0, concat_axis=0, tiled=True)


def partner(value, axis, mask):
    size = lax.axis_size(axis)
    return lax.ppermute(value, axis, [(m, m ^ mask) for m in range(size)])


def copies_kernel(share_ref, out_ref):
    for p in range(out_ref.shape[0]):
        out_ref[p] = share_ref[...]


def copies_of(share, members):
    return pl.pallas_call(
        copies_kernel,
        out_shape=jax.ShapeDtypeStruct((members, *share.shape), F32),
        name="copies",
    )(share)


def any_spec():
    return pl.BlockSpec(memory_space=pl.ANY)


def column(row, lanes):
    return jnp.broadcast_to(row, (lanes, lanes)).T


def picked_rows(rows, table_ref):
    nodes, lanes = table_ref.shape
    wide = 256
    col = jnp.concatenate([column(r, lanes) for r in rows], axis=0)
    off = col - lax.broadcasted_iota(jnp.int32, col.shape, 1)
    acc = jnp.zeros(col.shape, F32)
    for c in range(nodes // wide):
        hot = jnp.concatenate(
            [
                jnp.where(off == c * wide + k * lanes, F32(1), F32(0)).astype(BF16)
                for k in range(wide // lanes)
            ],
            axis=1,
        )
        acc += jnp.dot(hot, table_ref[c * wide : (c + 1) * wide, :], preferred_element_type=F32)
    return acc.astype(BF16)


def bound_kernel(rows_ref, table_ref, out_ref, halves, sems, *, tile):
    offered = rows_ref.shape[1] // tile
    got = picked_rows([rows_ref[:, k * tile : (k + 1) * tile] for k in range(offered)], table_ref)
    half = tile // 2
    for c in range(2):
        for k in range(offered):
            halves[c, k] = got[k * tile + c * half : k * tile + (c + 1) * half]
    copies = [
        pltpu.make_async_copy(halves.at[p % 2], out_ref.at[p], sems.at[p])
        for p in range(out_ref.shape[0])
    ]
    for c in copies:
        c.start()
    for c in copies:
        c.wait()


def bound_halves(rows, table, members, tile):
    offered = rows.shape[1] // tile
    width = table.shape[1]
    return pl.pallas_call(
        functools.partial(bound_kernel, tile=tile),
        out_specs=any_spec(),
        out_shape=jax.ShapeDtypeStruct((members, offered, tile // 2, width), BF16),
        scratch_shapes=[
            pltpu.VMEM((2, offered, tile // 2, width), BF16),
            pltpu.SemaphoreType.DMA((members,)),
        ],
        name="bound_halves",
    )(rows, table)


def stale_kernel(rows_ref, table_ref, *out_refs):
    lanes = table_ref.shape[1]
    count = rows_ref.shape[1] // lanes
    groups = len(out_refs)
    here = lax.axis_index("group")
    for k in range(groups):
        g = lax.rem(here + k, groups)
        rows = rows_ref[pl.ds(g, 1), :]
        out_refs[k][...] = picked_rows(
            [rows[:, c * lanes : (c + 1) * lanes] for c in range(count)], table_ref
        )


def stale_rows_sent(rows, table):
    groups, count = rows.shape
    vmem = pl.BlockSpec(memory_space=pltpu.VMEM)
    piece = jax.ShapeDtypeStruct((count, table.shape[1]), BF16)
    return pl.pallas_call(
        stale_kernel,
        in_specs=[vmem, vmem],
        out_specs=[vmem] * groups,
        out_shape=[piece] * groups,
        compiler_params=pltpu.CompilerParams(vmem_limit_bytes=12 * MIB),
        name="stale_rows_sent",
    )(rows, table)


def forward_kernel(
    src_ref, picks_ref, tiles_ref, own_ref, near_ref, far_ref, deg_ref, cot_ref, ws_ref,
    wn_ref, *refs, group, groups,
):
    stale_refs, refs = refs[:groups], refs[groups:]
    out_ref, dpre_t_ref, back_t_ref, part_out, *refs = refs
    tiles, sources, cots, aggs, outs, dpre_ts, back_ts, w_cat, inv, part_acc, *refs = refs
    part_ref, tile_sems, in_sems, out_sems, part_sem = refs
    blocks, tile, width = own_ref.shape
    tiles_row = src_ref.shape[0]
    members, offered, half, _ = near_ref.shape
    halo = members * offered
    stale = stale_refs[0].shape[0]
    core = lax.rem(lax.axis_index("member"), 2)
    here = lax.axis_index("group")

    def tile_copy(b):
        at = pl.ds(b * tiles_row, tiles_row)
        return pltpu.make_async_copy(tiles_ref.at[at], tiles.at[at], tile_sems.at[b])

    def halo_rows(which):
        return sources.at[pl.ds(blocks, halo), pl.ds(pl.multiple_of(which * half, half), half)]

    ins = [
        pltpu.make_async_copy(own_ref, sources.at[pl.ds(0, blocks)], in_sems.at[0]),
        pltpu.make_async_copy(near_ref.reshape(halo, half, width), halo_rows(core), in_sems.at[1]),
        pltpu.make_async_copy(far_ref.reshape(halo, half, width), halo_rows(1 - core), in_sems.at[2]),
        *[
            pltpu.make_async_copy(
                ref, sources.at[pl.ds(blocks + halo + k * stale, stale)], in_sems.at[3 + k]
            )
            for k, ref in enumerate(stale_refs)
        ],
    ]
    cot_in = pltpu.make_async_copy(cot_ref, cots, in_sems.at[3 + groups])
    for c in ins:
        c.start()
    tile_copy(0).start()
    cot_in.start()

    @pl.loop(1, blocks)
    def _(b):
        tile_copy(b).start()

    w_cat[:width, :] = ws_ref[...]
    w_cat[width:, :] = wn_ref[...]
    inv[...] = 1.0 / deg_ref[...].astype(F32)
    part_acc[...] = jnp.zeros_like(part_acc)
    for c in ins:
        c.wait()

    def source_of(b, t):
        s = src_ref[t, b]
        m = jnp.clip(s - blocks, 0, members - 1)
        near = blocks + m * offered + picks_ref[0, m]
        late = jnp.maximum(s - blocks - members, 0)
        from_group = late // stale
        back = here - from_group
        back = jnp.where(back < 0, back + groups, back)
        old = blocks + halo + back * stale + late - from_group * stale
        return jnp.where(s < blocks, s, jnp.where(s < blocks + members, near, old))

    outputs = ((outs, out_ref), (dpre_ts, dpre_t_ref), (back_ts, back_t_ref))

    def out_copies(g):
        at = pl.ds(g * group, group)
        return [
            pltpu.make_async_copy(buf.at[at], ref.at[at], out_sems.at[k, g])
            for k, (buf, ref) in enumerate(outputs)
        ]

    def arrived(g):
        for k in range(group):
            tile_copy(g * group + k).wait()

    def aggregate(g):
        for k in range(group):
            b = g * group + k
            lhs = jnp.concatenate(
                [tiles[b * tiles_row + t] for t in range(tiles_row)], axis=1
            )
            rhs = jnp.concatenate([sources[source_of(b, t)] for t in range(tiles_row)], axis=0)
            summed = jnp.dot(lhs, rhs, preferred_element_type=F32)
            aggs[b] = (summed * column(inv[pl.ds(b, 1), :], tile)).astype(BF16)

    def dense(g):
        at = pl.ds(g * group, group)
        rows = group * tile
        x = jnp.concatenate(
            [sources[at].reshape(rows, width), aggs[at].reshape(rows, width)], axis=1
        )
        pre = jnp.dot(x, w_cat[...], preferred_element_type=F32)
        scale = lax.rsqrt(jnp.mean(pre * pre, axis=-1, keepdims=True) + 1e-05)
        outs[at] = (pre * scale).astype(BF16).reshape(group, tile, width)
        grad = cots[at].reshape(rows, width).astype(F32)
        mix = jnp.mean(grad * pre, axis=-1, keepdims=True)
        dpre = (scale * grad - pre * (scale * scale * scale * mix)).astype(BF16)
        dpre_t = jnp.concatenate(
            [dpre[k * tile : (k + 1) * tile].T for k in range(group)], axis=1
        )
        inv_row = jnp.concatenate([inv[pl.ds(g * group + k, 1), :] for k in range(group)], axis=1)
        back = jnp.dot(wn_ref[...], dpre_t, preferred_element_type=F32) * inv_row
        part_acc[...] += jnp.dot(dpre_t, x, preferred_element_type=F32)
        for k in range(group):
            dpre_ts[g * group + k] = dpre_t[:, k * tile : (k + 1) * tile]
            back_ts[g * group + k] = back[:, k * tile : (k + 1) * tile].astype(BF16)

    last = blocks // group - 1
    arrived(0)
    aggregate(0)
    cot_in.wait()

    @pl.loop(1, last + 1)
    def _(g):
        arrived(g)
        dense(g - 1)
        aggregate(g)
        for c in out_copies(g - 1):
            c.start()

    dense(last)
    for c in out_copies(last):
        c.start()

    each = 2 * width // members
    for q in range(2):
        grad = part_acc[:, q * width : (q + 1) * width].T
        for p in range(members // 2):
            part_ref[q * (members // 2) + p, :each] = grad[p * each : (p + 1) * each]
    for p in range(members):
        part_ref[p, each:] = jnp.full((each, width), picks_ref[0, p].astype(F32), F32)
    part_copy = pltpu.make_async_copy(part_ref, part_out, part_sem)
    part_copy.start()

    @pl.loop(0, blocks // group)
    def _(g):
        for c in out_copies(g):
            c.wait()

    part_copy.wait()


def forward(src, picks, tiles, own, near, far, stale, degree, cot, w_self, w_neigh, group=4):
    blocks, tile, width = own.shape
    members, offered = near.shape[:2]
    groups = len(stale)
    count = blocks + members * offered + groups * stale[0].shape[0]
    smem = pl.BlockSpec(memory_space=pltpu.SMEM)
    vmem = pl.BlockSpec(memory_space=pltpu.VMEM)
    node = pltpu.VMEM((blocks, tile, width), BF16)
    return pl.pallas_call(
        functools.partial(forward_kernel, group=group, groups=groups),
        in_specs=[smem] * 2 + [any_spec()] * 4 + [vmem, any_spec(), vmem, vmem] + [any_spec()] * groups,
        out_specs=[any_spec()] * 4,
        scratch_shapes=[
            pltpu.VMEM(tiles.shape, BF16),
            pltpu.VMEM((count, tile, width), BF16),
            node,
            node,
            node,
            node,
            node,
            pltpu.VMEM((2 * width, width), BF16),
            pltpu.VMEM((blocks, tile), F32),
            pltpu.VMEM((width, 2 * width), F32),
            pltpu.VMEM((members, 4 * width // members, width), F32),
            pltpu.SemaphoreType.DMA((blocks,)),
            pltpu.SemaphoreType.DMA((4 + groups,)),
            pltpu.SemaphoreType.DMA((3, blocks // group)),
            pltpu.SemaphoreType.DMA,
        ],
        out_shape=[
            pltpu.HBM(own.shape, BF16),
            pltpu.HBM(own.shape, BF16),
            pltpu.HBM(own.shape, BF16),
            pltpu.HBM((members, 4 * width // members, width), F32),
        ],
        compiler_params=pltpu.CompilerParams(vmem_limit_bytes=40 * MIB),
        name="forward",
    )(src, picks, tiles, own, near, far, degree, cot, w_self, w_neigh, *stale)


def backward_kernel(
    src_ref, tiles_ref, back_ref, halo_ref, own_ref, tiles, backs, even, odd, halos,
    tile_sems, in_sem, out_sems, *, group,
):
    blocks, width, tile = back_ref.shape
    tiles_row = src_ref.shape[0]
    halo = halo_ref.shape[0]

    def tile_copy(b):
        at = pl.ds(b * tiles_row, tiles_row)
        return pltpu.make_async_copy(tiles_ref.at[at], tiles.at[at], tile_sems.at[b])

    back_in = pltpu.make_async_copy(back_ref, backs, in_sem)
    back_in.start()

    @pl.loop(0, blocks)
    def _(b):
        tile_copy(b).start()

    @pl.loop(0, even.shape[0])
    def _(s):
        even[s] = jnp.zeros((width, tile), F32)
        odd[s] = jnp.zeros((width, tile), F32)

    back_in.wait()

    @pl.loop(0, blocks, step=group)
    def _(first):
        for k in range(group):
            tile_copy(first + k).wait()
        for k in range(group):
            b = first + k
            back = backs[b]
            for t in range(0, tiles_row, 2):
                at = b * tiles_row + t
                pair = jnp.concatenate([tiles[at], tiles[at + 1]], axis=1)
                got = jnp.dot(back, pair, preferred_element_type=F32)
                even[src_ref[t, b]] += got[:, :tile]
                odd[src_ref[t + 1, b]] += got[:, tile:]

    @pl.loop(0, halo, step=4)
    def _(s):
        for k in range(4):
            halos[s + k] = (even[blocks + s + k] + odd[blocks + s + k]).astype(BF16)

    halo_out = pltpu.make_async_copy(halos, halo_ref, out_sems.at[0])
    halo_out.start()

    @pl.loop(0, blocks, step=4)
    def _(s):
        for k in range(4):
            even[s + k] += odd[s + k]

    own_out = pltpu.make_async_copy(even.at[pl.ds(0, blocks)], own_ref, out_sems.at[1])
    own_out.start()
    halo_out.wait()
    own_out.wait()


def backward(src, tiles, back_t, halo, count, group=4):
    blocks, width, tile = back_t.shape
    grads = pltpu.HBM((blocks, width, tile), F32)
    return pl.pallas_call(
        functools.partial(backward_kernel, group=group),
        in_specs=[pl.BlockSpec(memory_space=pltpu.SMEM), any_spec(), any_spec()],
        out_specs=[any_spec()] * 2,
        scratch_shapes=[
            pltpu.VMEM(tiles.shape, BF16),
            pltpu.VMEM(back_t.shape, BF16),
            pltpu.VMEM((count, width, tile), F32),
            pltpu.VMEM((count, width, tile), F32),
            pltpu.VMEM((halo, width, tile), BF16),
            pltpu.SemaphoreType.DMA((blocks,)),
            pltpu.SemaphoreType.DMA,
            pltpu.SemaphoreType.DMA((2,)),
        ],
        out_shape=[jax.ShapeDtypeStruct((halo, width, tile), BF16), grads],
        name="backward",
    )(src, tiles, back_t)


def local_kernel(acc_ref, dpre_ref, w_ref, out_ref):
    blocks, _, tile = acc_ref.shape

    @pl.loop(0, blocks, step=4)
    def _(first):
        for k in range(4):
            b = first + k
            both = acc_ref[b] + jnp.dot(w_ref[...], dpre_ref[b], preferred_element_type=F32)
            out_ref[pl.ds(b * tile, tile), :] = both.T


def local_rows(acc, dpre_t, w_self):
    blocks, width, tile = acc.shape
    return pl.pallas_call(
        local_kernel,
        out_shape=jax.ShapeDtypeStruct((blocks * tile, width), F32),
        compiler_params=pltpu.CompilerParams(vmem_limit_bytes=12 * MIB),
        name="local_rows",
    )(acc, dpre_t, w_self)


def final_kernel(
    parts_ref, returned_ref, rows_ref, local_ref, out_ref, spread, outs, sems, *, offered, chunk
):
    nodes, width = local_ref.shape
    members, _, tile = returned_ref.shape
    each = parts_ref.shape[1] // 2
    sums = [jnp.zeros((width, tile), F32) for _ in range(offered)]
    for p in range(members):
        block = returned_ref[p].astype(F32)
        wanted = parts_ref[p, each : each + 1, :]
        for k in range(offered):
            sums[k] += jnp.where(wanted == F32(k), block, F32(0))
    grad = jnp.concatenate([s.T for s in sums], axis=0)
    high = grad.astype(BF16)
    spread[:, :width] = high
    spread[:, width:] = (grad - high.astype(F32)).astype(BF16)
    copies = []
    for c in range(nodes // chunk):
        at = lax.broadcasted_iota(jnp.int32, (chunk, offered * tile), 0) + c * chunk
        hot = jnp.where(at == rows_ref[...], F32(1), F32(0)).astype(BF16)
        more = jnp.dot(hot, spread[...], preferred_element_type=F32)
        rows = slice(c * chunk, (c + 1) * chunk)
        outs[rows, :] = (local_ref[rows, :] + (more[:, :width] + more[:, width:])).astype(BF16)
        at = pl.ds(c * chunk, chunk)
        copies.append(pltpu.make_async_copy(outs.at[at], out_ref.at[at], sems.at[c]))
        copies[-1].start()
    for c in copies:
        c.wait()


def final(parts, returned, rows, local, offered, chunk=512):
    nodes, width = local.shape
    tile = returned.shape[2]
    return pl.pallas_call(
        functools.partial(final_kernel, offered=offered, chunk=chunk),
        out_specs=any_spec(),
        out_shape=jax.ShapeDtypeStruct((nodes, width), BF16),
        scratch_shapes=[
            pltpu.VMEM((offered * tile, 2 * width), BF16),
            pltpu.VMEM((nodes, width), BF16),
            pltpu.SemaphoreType.DMA((nodes // chunk,)),
        ],
        compiler_params=pltpu.CompilerParams(vmem_limit_bytes=12 * MIB),
        name="final",
    )(parts, returned, rows, local)


def on_device(
    features,
    history,
    tiles,
    tile_src,
    degree,
    boundary_rows,
    picks,
    stale_rows,
    w_self,
    w_neigh,
    cotangent,
):
    members = lax.axis_size("member")
    groups = lax.axis_size("group")
    tile = tiles.shape[1]
    width = features.shape[1]
    blocks = features.shape[0] // tile
    offered = boundary_rows.shape[1] // tile
    src = tile_src.T
    halves = bound_halves(boundary_rows, features, members, tile)
    near = exchange(halves, "member")
    stale_rows, halves = lax.optimization_barrier((stale_rows, halves))
    stale = list(stale_rows_sent(stale_rows, history))
    for k in range(1, groups):
        stale[k] = lax.ppermute(stale[k], "group", [(g, (g + k) % groups) for g in range(groups)])
    near, *stale = lax.optimization_barrier((near, *stale))
    far = lax.ppermute(near, "member", [(m, m ^ 1) for m in range(members)])
    stale = [piece.reshape(-1, tile, width) for piece in stale]
    own = features.reshape(blocks, tile, width)
    tiles = pltpu.with_memory_space_constraint(tiles, pltpu.HBM)
    out, dpre_t, back_t, part = forward(
        src,
        picks.reshape(1, -1),
        tiles,
        own,
        near,
        far,
        stale,
        degree.reshape(blocks, tile),
        cotangent.reshape(blocks, tile, width),
        w_self,
        w_neigh,
    )
    parts = exchange(part, "member")
    count = blocks + members + groups * stale[0].shape[0]
    halo_grad, own_grad = backward(src, tiles, back_t, members, count)
    parts, halo_grad, own_grad = lax.optimization_barrier((parts, halo_grad, own_grad))
    factor = 1.0 / math.sqrt(features.shape[0] * members * groups)
    returned = exchange(halo_grad, "member")
    share = parts[:, : parts.shape[1] // 2].sum(axis=0) * factor
    seen = [share] + [partner(share, "group", k) for k in range(1, groups)]
    while len(seen) > 1:
        seen = [a + b for a, b in zip(seen[::2], seen[1::2])]
    copies = copies_of(seen[0], members)
    returned, copies = lax.optimization_barrier((returned, copies))
    full = exchange(copies, "member").reshape(-1, width)
    local = local_rows(own_grad, dpre_t, w_self)
    grad_features = final(parts, returned, boundary_rows, local, offered)
    grad_self, grad_neigh = full[:width], full[width:]
    return (out.reshape(-1, width), grad_features, grad_self, grad_neigh)


def solution(mesh):
    placed = (
        P(("group", "member"), None),
        P(("group", "member"), None),
        P(("group", "member"), None, None),
        P(("group", "member"), None),
        P(("group", "member")),
        P(("group", "member"), None),
        P(("group", "member"), None),
        P(("group", "member"), None),
        P(),
        P(),
        P(("group", "member"), None),
    )
    return jax.shard_map(
        on_device,
        mesh=mesh,
        in_specs=placed,
        out_specs=(P(("group", "member"), None), P(("group", "member"), None), P(), P()),
        check_vma=False,
    )
```
